32 devices in a mesh: mc: 8 (over z, x), mr: 4 (over y, core).
Axes of the slice: x: 2, y: 2, z: 4, core: 2. Of those that a mesh axis runs over, the one named last changes fastest.
Arguments:
- column_panel: float32 [4096, 256], P('mc', 'mr'), may hold values from -0.375 to 0.375
- diag_block: float32 [256, 256], P('mc', 'mr'), may hold values from -4.3 to 4.3, as said below
- row_panel: float32 [256, 32768], P('mc', 'mr'), may hold values from -6 to 6
- trailing: float32 [4096, 32768], P('mc', 'mr'), may hold values from -6 to 6
Outputs:
- solved_panel: float32 [4096, 256], P('mc', 'mr')
- inverse_block: float32 [256, 256], P('mc', 'mr')
- scaled_panel: float32 [256, 32768], P('mc', 'mr')
- updated: float32 [4096, 32768], P('mc', 'mr')
The draws below stay inside these ranges and needn't reach their ends.
Inputs may be any that keep to these rules, and one draw needn't show every extreme that they name: `diag_block`: upper triangle with a diagonal of magnitude 2 to 4 and small off-diagonal entries.
All inputs are finite; a program needn't handle non-finite values.
Results may differ from the reference program's by a relative error of at most 0.00011.
Values sent between devices are 32-bit elements; how exact they have to be, the bound alone decides.
A program may use at most 128 MiB of HBM per device.

```python
import jax
import jax.numpy as jnp
from jax import lax

B = 256
COLS = 32768
ROWS = 4096


def draw_diag_block(key, part):
    first, second, third = jax.random.split(key, 3)
    offdiag = 0.06 * jnp.clip(jax.random.normal(first, (B, B), jnp.float32), -5.0, 5.0)
    signs = jnp.where(jax.random.bernoulli(second, 0.5, (B,)), 1.0, -1.0).astype(jnp.float32)
    magnitude = jax.random.uniform(third, (B,), jnp.float32, 2.0, 4.0)
    keep = 1.0 - jnp.eye(B, dtype=jnp.float32)
    return offdiag * keep + jnp.diag(signs * magnitude)


def shard_levels(rng, extent, cuts, smallest, largest):
    loudness = 1.0
    for position, parts in cuts:
        steps = jax.random.uniform(jax.random.fold_in(jax.random.fold_in(rng, 6), position), (parts,), jnp.float32, smallest / len(cuts), largest / len(cuts))
        loudness = loudness * jnp.repeat(jnp.exp(steps), extent[position] // parts).reshape((-1,) + (1,) * (len(extent) - 1 - position))
    return loudness


def centred(rng, shape, deviation, reach, pieces=(), kind=jnp.bfloat16):
    array = deviation * jax.random.normal(rng, shape, jnp.float32)
    if pieces:
        array = array * shard_levels(rng, shape, pieces, -0.22, 0.18)
    return jnp.clip(array, -reach, reach).astype(kind)


def setup_inputs(seed: int = 0) -> dict:
    key_of = jax.random.split(jax.random.key(seed), 5)
    column_panel = centred(key_of[0], (ROWS, B), B ** -0.5, 0.375, ((0, 8), (1, 4)), jnp.float32)
    diag_block = draw_diag_block(jax.random.fold_in(key_of[4], 71), 0)
    row_panel = centred(key_of[2], (B, COLS), 1.0, 6.0, ((0, 8), (1, 4)), jnp.float32)
    trailing = centred(key_of[3], (ROWS, COLS), 1.0, 6.0, ((0, 8), (1, 4)), jnp.float32)
    return {"column_panel": column_panel, "diag_block": diag_block, "row_panel": row_panel, "trailing": trailing}


def reference(column_panel, diag_block, row_panel, trailing):
    upper = jnp.triu(diag_block)
    identity = jnp.eye(B, dtype=diag_block.dtype)
    inverse_block = jax.scipy.linalg.solve_triangular(upper, identity, lower=False)
    solved_panel = -jnp.dot(column_panel, inverse_block, precision=lax.Precision.HIGHEST)
    updated = trailing + jnp.dot(solved_panel, row_panel, precision=lax.Precision.HIGHEST)
    scaled_panel = jnp.dot(inverse_block, row_panel, precision=lax.Precision.HIGHEST)
    return (solved_panel, inverse_block, scaled_panel, updated)
```

```python
import functools

import jax
import jax.numpy as jnp
from jax import lax
from jax.experimental import pallas as pl
from jax.experimental.pallas import tpu as pltpu
from jax.sharding import PartitionSpec as P

VMEM_BYTES = 67043328
HIGHEST = lax.Precision.HIGHEST


def dot(a, b):
    return jnp.dot(a, b, precision=HIGHEST, preferred_element_type=jnp.float32)


def upper_inverse(matrix):
    order = matrix.shape[0]
    row = lax.broadcasted_iota(jnp.int32, (order, order), 0)
    col = lax.broadcasted_iota(jnp.int32, (order, order), 1)
    on_diag = row == col
    pivots = jnp.where(on_diag, matrix, 0.0)
    recip_col = 1.0 / jnp.sum(pivots, axis=1, keepdims=True)
    recip_row = 1.0 / jnp.sum(pivots, axis=0, keepdims=True)
    power = -(recip_col * jnp.where(col > row, matrix, 0.0))
    identity = jnp.where(on_diag, 1.0, 0.0)
    product = identity + power
    steps = max((order - 1).bit_length(), 1)
    for level in range(steps - 1):
        power = dot(power, power)
        product = dot(product, identity + power)
    return product * recip_row


def split(value):
    high = value.astype(jnp.bfloat16)
    low = (value - high.astype(jnp.float32)).astype(jnp.bfloat16)
    return high, low


def kernel(n_mc, n_mr, chunks, tile,
           column_ref, diag_ref, row_ref, trailing_ref,
           solved_ref, inverse_ref, scaled_ref, updated_ref,
           panel, columns, diags, matrix, flipped, left_high, left_low,
           load_sem, row_sem, trail_sem, send_sem, recv_sem,
           diag_send, diag_recv, block_send, block_recv, col_send, col_recv):
    mc = lax.axis_index("mc")
    mr = lax.axis_index("mr")
    levels = n_mc // 2
    z = mc // 2
    x = lax.rem(mc, 2)
    rows = row_ref.shape[0]
    half = rows // 2
    cols = row_ref.shape[1]
    width = cols // chunks
    block_cols = diag_ref.shape[1]
    height = column_ref.shape[1]

    def at(mc_index, mr_index):
        return {"mc": mc_index, "mr": mr_index}

    down = jnp.maximum(mc - 2, 0)
    up = jnp.minimum(mc + 2, n_mc - 1)
    across = z * 2 + 1 - x
    other = 1 - x
    top = 2 * (levels - 1) + other
    bottom = other

    barrier = pltpu.get_barrier_semaphore()

    def greet(mc_index, mr_index):
        pl.semaphore_signal(barrier, inc=1, device_id=at(mc_index, mr_index),
                            device_id_type=pl.DeviceIdType.MESH)

    @pl.when(z > 0)
    def _():
        greet(down, mr)

    @pl.when(z < levels - 1)
    def _():
        greet(up, mr)

    greet(across, mr)
    for step in range(1, n_mr):
        greet(mc, lax.rem(mr + step, n_mr))

    own_diag = pltpu.make_async_copy(
        diag_ref, diags.at[mr, pl.ds(pl.multiple_of(mc * rows, rows), rows)], load_sem.at[0])
    own_part = lambda k: pl.ds(pl.multiple_of(k * block_cols, block_cols), block_cols)
    own_column = pltpu.make_async_copy(column_ref, columns.at[own_part(mr)], load_sem.at[1])

    def own_row(c):
        part = pl.ds(pl.multiple_of(c * width, width), width)
        return pltpu.make_async_copy(
            row_ref.at[:, part], panel.at[pl.ds(pl.multiple_of(mc * rows, rows), rows), part], row_sem.at[c])

    own_diag.start()
    for c in range(chunks):
        own_row(c).start()
    own_column.start()
    pl.semaphore_wait(barrier, n_mr + jnp.where(z > 0, 1, 0) + jnp.where(z < levels - 1, 1, 0))

    def piece(shard, c, low=None):
        first = pl.multiple_of(shard * rows, rows)
        count = rows
        if low is not None:
            first = pl.multiple_of(shard * rows + low * half, half)
            count = half
        return panel.at[pl.ds(first, count), pl.ds(pl.multiple_of(c * width, width), width)]

    def copy(shard, c, way, slot, target, low=None):
        ref = piece(shard, c, low)
        return pltpu.make_async_remote_copy(
            src_ref=ref, dst_ref=ref,
            send_sem=send_sem.at[way, slot, c],
            recv_sem=recv_sem.at[2 * shard + (1 if low == 1 else 0), c],
            device_id=at(target, mr), device_id_type=pl.DeviceIdType.MESH)

    def diag_copy(shard, way, slot, target):
        ref = diags.at[mr, pl.ds(pl.multiple_of(shard * rows, rows), rows)]
        return pltpu.make_async_remote_copy(
            src_ref=ref, dst_ref=ref, send_sem=diag_send.at[way, slot], recv_sem=diag_recv.at[shard],
            device_id=at(target, mr), device_id_type=pl.DeviceIdType.MESH)

    def block_copy(step, source, target):
        ref = diags.at[source]
        return pltpu.make_async_remote_copy(
            src_ref=ref, dst_ref=ref, send_sem=block_send.at[step], recv_sem=block_recv.at[step],
            device_id=at(mc, target), device_id_type=pl.DeviceIdType.MESH)

    def column_copy(step, source, target):
        ref = columns.at[own_part(source)]
        return pltpu.make_async_remote_copy(
            src_ref=ref, dst_ref=ref, send_sem=col_send.at[step], recv_sem=col_recv.at[step],
            device_id=at(mc, target), device_id_type=pl.DeviceIdType.MESH)

    def send_row(c):
        own_row(c).wait()

        @pl.when(z > 0)
        def _():
            copy(mc, c, 0, z, down).start()

        @pl.when(z < levels - 1)
        def _():
            copy(mc, c, 1, z, up).start()

        copy(mc, c, 2, z, across).start()

    own_diag.wait()

    @pl.when(z > 0)
    def _():
        diag_copy(mc, 0, z, down).start()

    @pl.when(z < levels - 1)
    def _():
        diag_copy(mc, 1, z, up).start()

    diag_copy(mc, 2, z, across).start()
    send_row(0)
    own_column.wait()
    for step in range(1, n_mr):
        column_copy(step, mr, lax.rem(mr + step, n_mr)).start()

    def trail_copy(c):
        part = pl.ds(pl.multiple_of(c * width, width), width)
        return pltpu.make_async_copy(trailing_ref.at[:, part], updated_ref.at[:, part], trail_sem.at[c])

    @pl.loop(0, chunks)
    def _(c):
        trail_copy(c).start()

    first_half_only = lambda q: jnp.logical_or(
        jnp.logical_and(q == levels - 1, z != levels - 1), jnp.logical_and(q == 0, z != 0))

    def each_across(q, c, act):
        @pl.when(first_half_only(q))
        def _():
            act(copy(2 * q + x, c, 2, q, across, 0))

        @pl.when(jnp.logical_not(first_half_only(q)))
        def _():
            act(copy(2 * q + x, c, 2, q, across))

    start = lambda d: d.start()

    for hop in range(levels - 1):
        above = z + 1 + hop
        below = z - 1 - hop

        @pl.when(above < levels)
        def _():
            diag_copy(2 * above + x, 0, above, down).wait_recv()

            @pl.when(z > 0)
            def _():
                diag_copy(2 * above + x, 0, above, down).start()

            diag_copy(2 * above + x, 2, above, across).start()

        @pl.when(below >= 0)
        def _():
            diag_copy(2 * below + x, 1, below, up).wait_recv()

            @pl.when(z < levels - 1)
            def _():
                diag_copy(2 * below + x, 1, below, up).start()

            diag_copy(2 * below + x, 2, below, across).start()

        if hop + 1 < chunks:
            send_row(hop + 1)
    for c in range(levels, chunks):
        send_row(c)

    def invert():
        for q in range(levels):
            diag_copy(2 * q + other, 2, q, across).wait_recv()
        for step in range(1, n_mr):
            block_copy(step, mr, lax.rem(mr + step, n_mr)).start()
        for step in range(1, n_mr):
            block_copy(step, lax.rem(mr + n_mr - step, n_mr), lax.rem(mr + step, n_mr)).wait_recv()
        for k in range(n_mr):
            matrix[:, k * block_cols:(k + 1) * block_cols] = diags[k]
        matrix[...] = upper_inverse(matrix[...])
        own_inverse = matrix[pl.ds(pl.multiple_of(mc * rows, rows), rows), :]
        for step in range(1, n_mr):
            column_copy(step, lax.rem(mr + n_mr - step, n_mr), lax.rem(mr + step, n_mr)).wait_recv()
        flipped[...] = -lax.dot_general(
            matrix[...], columns[...], (((0,), (0,)), ((), ())),
            precision=HIGHEST, preferred_element_type=jnp.float32)
        solved_ref[...] = flipped[own_part(mr), :]
        left_high[0:height, :], left_low[0:height, :] = split(flipped[...].T)
        left_high[height:height + rows, :], left_low[height:height + rows, :] = split(own_inverse)
        for k in range(n_mr):
            @pl.when(mr == k)
            def _():
                inverse_ref[...] = own_inverse[:, k * block_cols:(k + 1) * block_cols]

    for phase in range(levels - 1):
        if phase == min(1, levels - 2):
            invert()

        above = z + 1 + phase
        below = z - 1 - phase

        @pl.loop(0, chunks)
        def _(c):
            @pl.when(above < levels)
            def _():
                copy(2 * above + x, c, 0, above, down).wait_recv()

                @pl.when(z > 0)
                def _():
                    copy(2 * above + x, c, 0, above, down).start()

                each_across(above, c, start)

            @pl.when(below >= 0)
            def _():
                copy(2 * below + x, c, 1, below, up).wait_recv()

                @pl.when(z < levels - 1)
                def _():
                    copy(2 * below + x, c, 1, below, up).start()

                each_across(below, c, start)

            if phase == 0:
                copy(2 * z + other, c, 2, z, across).wait_recv()

                @pl.when(z == levels - 1)
                def _():
                    copy(top, c, 0, levels, down, 1).start()

                @pl.when(z == 0)
                def _():
                    copy(bottom, c, 1, levels, up, 1).start()

            @pl.when(above == levels)
            def _():
                @pl.when(z < levels - 1)
                def _():
                    copy(top, c, 0, levels, down, 1).wait_recv()

                    @pl.when(z > 0)
                    def _():
                        copy(top, c, 0, levels, down, 1).start()

            @pl.when(below == -1)
            def _():
                @pl.when(z > 0)
                def _():
                    copy(bottom, c, 1, levels, up, 1).wait_recv()

                    @pl.when(z < levels - 1)
                    def _():
                        copy(bottom, c, 1, levels, up, 1).start()

    @pl.loop(0, chunks)
    def _(c):
        trail_copy(c).wait()

        @pl.when(z == 0)
        def _():
            copy(top, c, 0, levels, down, 1).wait_recv()

        @pl.when(z == levels - 1)
        def _():
            copy(bottom, c, 1, levels, up, 1).wait_recv()

        for q in range(levels):
            def receive(low):
                copy(2 * q + other, c, 2, q, across, low).wait_recv()

            @pl.when(jnp.logical_and(z != q, first_half_only(q)))
            def _():
                receive(0)

            @pl.when(jnp.logical_and(z != q, jnp.logical_not(first_half_only(q))))
            def _():
                receive(None)

        for t in range(width // tile):
            part = pl.ds(pl.multiple_of(c * width + t * tile, tile), tile)
            right_high, right_low = split(panel[:, part])
            product = jnp.dot(left_high[...], right_low, preferred_element_type=jnp.float32)
            product += jnp.dot(left_low[...], right_high, preferred_element_type=jnp.float32)
            product += jnp.dot(left_high[...], right_high, preferred_element_type=jnp.float32)
            updated_ref[:, part] = updated_ref[:, part] + product[0:height]
            scaled_ref[:, part] = product[height:height + rows]

    for q in range(levels):
        @pl.when(jnp.logical_and(z > 0, z <= q))
        def _():
            diag_copy(2 * q + x, 0, q, down).wait_send()

        @pl.when(jnp.logical_and(z < levels - 1, z >= q))
        def _():
            diag_copy(2 * q + x, 1, q, up).wait_send()

        diag_copy(2 * q + x, 2, q, across).wait_send()
    for step in range(1, n_mr):
        block_copy(step, mr, lax.rem(mr + step, n_mr)).wait_send()
        column_copy(step, mr, lax.rem(mr + step, n_mr)).wait_send()

    @pl.loop(0, chunks)
    def _(c):
        for q in range(levels):
            @pl.when(jnp.logical_and(z > 0, z <= q))
            def _():
                copy(2 * q + x, c, 0, q, down).wait_send()

            @pl.when(jnp.logical_and(z < levels - 1, z >= q))
            def _():
                copy(2 * q + x, c, 1, q, up).wait_send()

            each_across(q, c, lambda d: d.wait_send())

        @pl.when(z > 0)
        def _():
            copy(top, c, 0, levels, down, 1).wait_send()

        @pl.when(z < levels - 1)
        def _():
            copy(bottom, c, 1, levels, up, 1).wait_send()


def store(*refs):
    sources, targets, sem = refs[:4], refs[4:8], refs[8]
    strips = sem.shape[0] - 3
    deep = sources[3].shape[0] // strips
    copies = []
    for i in range(strips):
        part = pl.ds(i * deep, deep)
        copies.append(pltpu.make_async_copy(sources[3].at[part], targets[3].at[part], sem.at[3 + i]))
    for i in range(3):
        copies.append(pltpu.make_async_copy(sources[i], targets[i], sem.at[i]))
    for c in copies:
        c.start()
    for c in copies:
        c.wait()


def shards(n_mc, n_mr, column_panel, diag_block, row_panel, trailing):
    rows, block_cols = diag_block.shape
    height, cols = trailing.shape
    order = rows * n_mc
    levels = n_mc // 2
    chunks = max(1, 16 // levels)
    while cols % (chunks * 128):
        chunks //= 2
    width = cols // chunks
    tile = 512 if width % 512 == 0 else 128
    held = 4 * (height * cols + rows * cols + block_cols * height + rows * 128) + 64 * 1024
    dma = pltpu.SemaphoreType.DMA
    f32 = jnp.float32
    anywhere = pl.BlockSpec(memory_space=pl.ANY)
    vmem = pl.BlockSpec(memory_space=pltpu.VMEM)
    parts = pl.pallas_call(
        functools.partial(kernel, n_mc, n_mr, chunks, tile),
        out_shape=(
            pltpu.VMEM((block_cols, height), f32),
            pltpu.VMEM(diag_block.shape, f32),
            pltpu.VMEM(row_panel.shape, f32),
            pltpu.VMEM(trailing.shape, f32),
        ),
        in_specs=[pl.BlockSpec(memory_space=pltpu.HBM)] * 4,
        out_specs=(vmem,) * 4,
        scratch_shapes=[
            pltpu.VMEM((order, cols), f32),
            pltpu.VMEM((order, height), f32),
            pltpu.VMEM((n_mr, order, block_cols), f32),
            pltpu.VMEM((order, order), f32),
            pltpu.VMEM((order, height), f32),
            pltpu.VMEM((height + rows, order), jnp.bfloat16),
            pltpu.VMEM((height + rows, order), jnp.bfloat16),
            dma((2,)), dma((chunks,)), dma((chunks,)),
            dma((3, levels + 1, chunks)), dma((2 * n_mc, chunks)),
            dma((3, levels)), dma((n_mc,)), dma((n_mr,)), dma((n_mr,)), dma((n_mr,)), dma((n_mr,)),
        ],
        compiler_params=pltpu.CompilerParams(
            collective_id=0, has_side_effects=True, vmem_limit_bytes=VMEM_BYTES - held),
    )(column_panel.T, diag_block, row_panel, trailing)
    solved, inverse, scaled, updated = pl.pallas_call(
        store,
        out_shape=tuple(jax.ShapeDtypeStruct(part.shape, f32) for part in parts),
        in_specs=[vmem] * 4,
        out_specs=(anywhere,) * 4,
        scratch_shapes=[dma((3 + 8,))],
        compiler_params=pltpu.CompilerParams(vmem_limit_bytes=1024 * 1024),
    )(*parts)
    return solved.T, inverse, scaled, updated


def solution(mesh):
    placed = (P("mc", "mr"),) * 4
    return jax.shard_map(
        functools.partial(shards, mesh.shape["mc"], mesh.shape["mr"]),
        mesh=mesh, in_specs=placed, out_specs=placed, check_vma=False)
```

```python
import functools

import jax
import jax.numpy as jnp
from jax import lax
from jax.experimental import pallas as pl
from jax.experimental.pallas import tpu as pltpu
from jax.sharding import PartitionSpec as P

VMEM_BYTES = 67043328
HIGHEST = lax.Precision.HIGHEST


def dot(a, b):
    return jnp.dot(a, b, precision=HIGHEST, preferred_element_type=jnp.float32)


def upper_inverse(matrix):
    order = matrix.shape[0]
    row = lax.broadcasted_iota(jnp.int32, (order, order), 0)
    col = lax.broadcasted_iota(jnp.int32, (order, order), 1)
    on_diag = row == col
    pivots = jnp.where(on_diag, matrix, 0.0)
    recip_col = 1.0 / jnp.sum(pivots, axis=1, keepdims=True)
    recip_row = 1.0 / jnp.sum(pivots, axis=0, keepdims=True)
    power = -(recip_col * jnp.where(col > row, matrix, 0.0))
    identity = jnp.where(on_diag, 1.0, 0.0)
    product = identity + power
    steps = max((order - 1).bit_length(), 1)
    for level in range(steps - 1):
        power = dot(power, power)
        product = dot(product, identity + power)
    return product * recip_row


def split(value):
    high = value.astype(jnp.bfloat16)
    low = (value - high.astype(jnp.float32)).astype(jnp.bfloat16)
    return high, low


def kernel(n_mc, n_mr, chunks, late, tile,
           column_ref, diag_ref, row_ref, trailing_ref,
           solved_ref, inverse_ref, scaled_ref, updated_ref, panel, left_high, left_low,
           columns, diags, matrix, flipped,
           load_sem, trail_sem, send_sem, line_recv, half_recv, pair_recv, rest_recv,
           diag_send, diag_recv, block_send, block_recv, col_send, col_recv):
    mc = lax.axis_index("mc")
    mr = lax.axis_index("mr")
    levels = n_mc // 2
    z = mc // 2
    x = lax.rem(mc, 2)
    rows = row_ref.shape[0]
    half = rows // 2
    cols = row_ref.shape[1]
    width = cols // chunks
    block_cols = diag_ref.shape[1]
    height = column_ref.shape[1]
    last = levels - 1

    def at(mc_index, mr_index):
        return {"mc": mc_index, "mr": mr_index}

    down = jnp.maximum(mc - 2, 0)
    up = jnp.minimum(mc + 2, n_mc - 1)
    across = z * 2 + 1 - x
    other = 1 - x
    top = 2 * last + other
    bottom = other

    barrier = pltpu.get_barrier_semaphore()

    def greet(mc_index, mr_index):
        pl.semaphore_signal(barrier, inc=1, device_id=at(mc_index, mr_index),
                            device_id_type=pl.DeviceIdType.MESH)

    @pl.when(z > 0)
    def _():
        greet(down, mr)

    @pl.when(z < last)
    def _():
        greet(up, mr)

    greet(across, mr)
    for step in range(1, n_mr):
        greet(mc, lax.rem(mr + step, n_mr))

    own_rows = pl.ds(pl.multiple_of(mc * rows, rows), rows)
    own_part = lambda k: pl.ds(pl.multiple_of(k * block_cols, block_cols), block_cols)
    own_diag = pltpu.make_async_copy(diag_ref, diags.at[mr, own_rows], load_sem.at[0])
    own_column = pltpu.make_async_copy(column_ref, columns.at[own_part(mr)], load_sem.at[1])
    own_first = pltpu.make_async_copy(
        row_ref.at[:, pl.ds(0, width)], panel.at[own_rows, pl.ds(0, width)], load_sem.at[2])
    own_diag.start()
    own_first.start()
    if chunks > 1:
        own_rest = pltpu.make_async_copy(
            row_ref.at[:, pl.ds(width, cols - width)], panel.at[own_rows, pl.ds(width, cols - width)],
            load_sem.at[3])
        own_rest.start()
    own_column.start()
    pl.semaphore_wait(barrier, n_mr + jnp.where(z > 0, 1, 0) + jnp.where(z < last, 1, 0))

    def remote(ref, send, recv, mc_index, mr_index):
        return pltpu.make_async_remote_copy(
            src_ref=ref, dst_ref=ref, send_sem=send, recv_sem=recv,
            device_id=at(mc_index, mr_index), device_id_type=pl.DeviceIdType.MESH)

    def piece(shard, c, low=None):
        first = pl.multiple_of(shard * rows, rows)
        count = rows
        if low is not None:
            first = pl.multiple_of(shard * rows + low * half, half)
            count = half
        return panel.at[pl.ds(first, count), pl.ds(pl.multiple_of(c * width, width), width)]

    target = (down, up, across)

    def line(q, c, way):
        return remote(piece(2 * q + x, c), send_sem.at[way], line_recv.at[q, c], target[way], mr)

    def split_piece(c, way):
        return remote(piece((top, bottom)[way], c, 1), send_sem.at[way], half_recv.at[way, c], target[way], mr)

    def pair(shard, c):
        return remote(piece(shard, c), send_sem.at[2], pair_recv.at[c], across, mr)

    def cross(q, c, low=None):
        return remote(piece(2 * q + x, c, low), send_sem.at[2], rest_recv.at[c], across, mr)

    def diag_line(q, way):
        ref = diags.at[mr, pl.ds(pl.multiple_of((2 * q + x) * rows, rows), rows)]
        return remote(ref, diag_send.at[way], diag_recv.at[q if way < 2 else levels], target[way], mr)

    def block_copy(k, step):
        return remote(diags.at[k], block_send.at[0], block_recv.at[0], mc, lax.rem(mr + step, n_mr))

    def column_copy(k, step):
        return remote(columns.at[own_part(k)], col_send.at[0], col_recv.at[0], mc, lax.rem(mr + step, n_mr))

    def send_row(c):
        @pl.when(z > 0)
        def _():
            line(z, c, 0).start()

        @pl.when(z < last)
        def _():
            line(z, c, 1).start()

        pair(mc, c).start()

    own_diag.wait()

    @pl.when(z > 0)
    def _():
        diag_line(z, 0).start()

    @pl.when(z < last)
    def _():
        diag_line(z, 1).start()

    diag_line(z, 2).start()
    own_first.wait()
    send_row(0)
    own_column.wait()
    for step in range(1, n_mr):
        column_copy(mr, step).start()
    if chunks > 1:
        own_rest.wait()
    load_trailing = pltpu.make_async_copy(trailing_ref, updated_ref, trail_sem.at[0])
    load_trailing.start()

    for hop in range(last):
        above = z + 1 + hop
        below = z - 1 - hop

        @pl.when(above < levels)
        def _():
            diag_line(above, 0).wait_recv()

            @pl.when(z > 0)
            def _():
                diag_line(above, 0).start()

            diag_line(above, 2).start()

        @pl.when(below >= 0)
        def _():
            diag_line(below, 1).wait_recv()

            @pl.when(z < last)
            def _():
                diag_line(below, 1).start()

            diag_line(below, 2).start()

        if hop + 1 < chunks:
            send_row(hop + 1)
    for c in range(levels, chunks):
        send_row(c)

    first_half_only = lambda q: jnp.logical_or(
        jnp.logical_and(q == last, z != last), jnp.logical_and(q == 0, z != 0))

    def send_across(q, c):
        @pl.when(first_half_only(q))
        def _():
            cross(q, c, 0).start()

        @pl.when(jnp.logical_not(first_half_only(q)))
        def _():
            cross(q, c).start()

    def invert():
        remote(diags.at[mr, pl.ds(0, levels * rows)], diag_send.at[2], diag_recv.at[levels], across, mr).wait_recv()
        for step in range(1, n_mr):
            block_copy(mr, step).start()
        remote(diags.at[pl.ds(0, n_mr - 1)], block_send.at[0], block_recv.at[0], mc, lax.rem(mr + 1, n_mr)).wait_recv()
        for k in range(n_mr):
            matrix[:, k * block_cols:(k + 1) * block_cols] = diags[k]
        matrix[...] = upper_inverse(matrix[...])
        own_inverse = matrix[own_rows, :]
        remote(columns.at[pl.ds(0, (n_mr - 1) * block_cols)], col_send.at[0], col_recv.at[0], mc,
               lax.rem(mr + 1, n_mr)).wait_recv()
        flipped[...] = -lax.dot_general(
            matrix[...], columns[...], (((0,), (0,)), ((), ())),
            precision=HIGHEST, preferred_element_type=jnp.float32)
        solved_ref[...] = flipped[own_part(mr), :]
        left_high[0:height, :], left_low[0:height, :] = split(flipped[...].T)
        left_high[height:height + rows, :], left_low[height:height + rows, :] = split(own_inverse)
        for k in range(n_mr):
            @pl.when(mr == k)
            def _():
                inverse_ref[...] = own_inverse[:, k * block_cols:(k + 1) * block_cols]

    for phase in range(last):
        if phase == min(1, levels - 2):
            invert()

        above = z + 1 + phase
        below = z - 1 - phase

        @pl.loop(0, chunks)
        def _(c):
            @pl.when(above < levels)
            def _():
                line(above, c, 0).wait_recv()

                @pl.when(z > 0)
                def _():
                    line(above, c, 0).start()

                send_across(above, c)

            @pl.when(below >= 0)
            def _():
                line(below, c, 1).wait_recv()

                @pl.when(z < last)
                def _():
                    line(below, c, 1).start()

                send_across(below, c)

            if phase == 0:
                pair(2 * z + other, c).wait_recv()

                @pl.when(z == last)
                def _():
                    split_piece(c, 0).start()

                @pl.when(z == 0)
                def _():
                    split_piece(c, 1).start()

            @pl.when(above == levels)
            def _():
                @pl.when(z < last)
                def _():
                    split_piece(c, 0).wait_recv()

                    @pl.when(z > 0)
                    def _():
                        split_piece(c, 0).start()

            @pl.when(below == -1)
            def _():
                @pl.when(z > 0)
                def _():
                    split_piece(c, 1).wait_recv()

                    @pl.when(z < last)
                    def _():
                        split_piece(c, 1).start()

    def receive_rest(c):
        @pl.when(z == 0)
        def _():
            split_piece(c, 0).wait_recv()

        @pl.when(z == last)
        def _():
            split_piece(c, 1).wait_recv()

        def gathered(halves):
            ref = panel.at[pl.ds(0, halves * half), pl.ds(0, width)]
            remote(ref, send_sem.at[2], rest_recv.at[c], across, mr).wait_recv()

        at_end = jnp.logical_or(z == 0, z == last)

        @pl.when(at_end)
        def _():
            gathered(2 * levels - 3)

        if levels > 2:
            @pl.when(jnp.logical_not(at_end))
            def _():
                gathered(2 * levels - 4)

    load_trailing.wait()

    @pl.loop(0, chunks - late)
    def _(c):
        receive_rest(c)
        for t in range(width // tile):
            part = pl.ds(pl.multiple_of(c * width + t * tile, tile), tile)
            product = multiply(left_high, left_low, panel[:, part])
            updated_ref[:, part] = updated_ref[:, part] + product[0:height]
            scaled_ref[:, part] = product[height:height + rows]

    for c in range(chunks - late, chunks):
        receive_rest(c)

    def sent(way, halves, diag_pieces):
        remote(panel.at[pl.ds(0, halves * half)], send_sem.at[way], pair_recv.at[0], target[way], mr).wait_send()
        remote(diags.at[mr, pl.ds(0, diag_pieces * rows)], diag_send.at[way], diag_recv.at[0], target[way],
               mr).wait_send()

    for k in range(levels):
        @pl.when(z == k)
        def _():
            if k > 0:
                sent(0, 2 * (levels - k) + 1, levels - k)
            if k < last:
                sent(1, 2 * (k + 1) + 1, k + 1)
            sent(2, 2 * levels - (1 if k in (0, last) else 2), levels)

    remote(diags.at[pl.ds(0, n_mr - 1)], block_send.at[0], block_recv.at[0], mc, lax.rem(mr + 1, n_mr)).wait_send()
    remote(columns.at[pl.ds(0, (n_mr - 1) * block_cols)], col_send.at[0], col_recv.at[0], mc,
           lax.rem(mr + 1, n_mr)).wait_send()


def multiply(left_high, left_low, right):
    right_high, right_low = split(right)
    product = jnp.dot(left_high[...], right_low, preferred_element_type=jnp.float32)
    product += jnp.dot(left_low[...], right_high, preferred_element_type=jnp.float32)
    return product + jnp.dot(left_high[...], right_high, preferred_element_type=jnp.float32)


def finish(done, tile, solved, inverse, scaled, updated, panel, left_high, left_low,
           solved_out, inverse_out, scaled_out, updated_out, held_updated, held_scaled, sem, tile_sem):
    height, cols = updated.shape
    strips = sem.shape[0] - 3
    deep = height // strips
    ready = pl.ds(0, done)
    copies = []
    for i in range(strips):
        part = pl.ds(i * deep, deep)
        copies.append(pltpu.make_async_copy(updated.at[part, ready], updated_out.at[part, ready], sem.at[3 + i]))
    copies.append(pltpu.make_async_copy(solved, solved_out, sem.at[0]))
    copies.append(pltpu.make_async_copy(inverse, inverse_out, sem.at[1]))
    copies.append(pltpu.make_async_copy(scaled.at[:, ready], scaled_out.at[:, ready], sem.at[2]))
    for c in copies:
        c.start()
    for t in range((cols - done) // tile):
        part = pl.ds(done + t * tile, tile)
        slot = pl.ds(t * tile, tile)
        product = multiply(left_high, left_low, panel[:, part])
        held_updated[:, slot] = updated[:, part] + product[0:height]
        held_scaled[:, slot] = product[height:]
        copies.append(pltpu.make_async_copy(held_updated.at[:, slot], updated_out.at[:, part], tile_sem.at[0, t]))
        copies.append(pltpu.make_async_copy(held_scaled.at[:, slot], scaled_out.at[:, part], tile_sem.at[1, t]))
        copies[-2].start()
        copies[-1].start()
    for c in copies:
        c.wait()


def shards(n_mc, n_mr, column_panel, diag_block, row_panel, trailing):
    rows, block_cols = diag_block.shape
    height, cols = trailing.shape
    order = rows * n_mc
    levels = n_mc // 2
    chunks = max(1, 16 // levels)
    while cols % (chunks * 128):
        chunks //= 2
    late = 1 if chunks > 1 else 0
    width = cols // chunks
    done = cols - late * width
    tile = 512 if width % 512 == 0 else 128
    held = 4 * (height * cols + rows * cols + block_cols * height + rows * 128 + order * cols
                + (height + rows) * order) + 64 * 1024
    dma = pltpu.SemaphoreType.DMA
    f32 = jnp.float32
    anywhere = pl.BlockSpec(memory_space=pl.ANY)
    vmem = pl.BlockSpec(memory_space=pltpu.VMEM)
    parts = pl.pallas_call(
        functools.partial(kernel, n_mc, n_mr, chunks, late, tile),
        out_shape=(
            pltpu.VMEM((block_cols, height), f32),
            pltpu.VMEM(diag_block.shape, f32),
            pltpu.VMEM(row_panel.shape, f32),
            pltpu.VMEM(trailing.shape, f32),
            pltpu.VMEM((order, cols), f32),
            pltpu.VMEM((height + rows, order), jnp.bfloat16),
            pltpu.VMEM((height + rows, order), jnp.bfloat16),
        ),
        in_specs=[pl.BlockSpec(memory_space=pltpu.HBM)] * 4,
        out_specs=(vmem,) * 7,
        scratch_shapes=[
            pltpu.VMEM((order, height), f32),
            pltpu.VMEM((n_mr, order, block_cols), f32),
            pltpu.VMEM((order, order), f32),
            pltpu.VMEM((order, height), f32),
            dma((4,)), dma((1,)), dma((3,)), dma((levels, chunks)), dma((2, chunks)), dma((chunks,)), dma((chunks,)),
            dma((3,)), dma((levels + 1,)), dma((1,)), dma((1,)), dma((1,)), dma((1,)),
        ],
        compiler_params=pltpu.CompilerParams(
            collective_id=0, has_side_effects=True, vmem_limit_bytes=VMEM_BYTES - held),
    )(column_panel.T, diag_block, row_panel, trailing)
    tiles = max(1, (cols - done) // tile)
    spare = max(tile, cols - done)
    solved, inverse, scaled, updated = pl.pallas_call(
        functools.partial(finish, done, tile),
        out_shape=tuple(jax.ShapeDtypeStruct(part.shape, f32) for part in parts[:4]),
        in_specs=[vmem] * 7,
        out_specs=(anywhere,) * 4,
        scratch_shapes=[pltpu.VMEM((height, spare), f32), pltpu.VMEM((rows, spare), f32), dma((3 + 8,)),
                        dma((2, tiles))],
        compiler_params=pltpu.CompilerParams(vmem_limit_bytes=4 * (height + rows) * (spare + 4 * tile) + 1024 * 1024),
    )(*parts)
    return solved.T, inverse, scaled, updated


def solution(mesh):
    placed = (P("mc", "mr"),) * 4
    return jax.shard_map(
        functools.partial(shards, mesh.shape["mc"], mesh.shape["mr"]),
        mesh=mesh, in_specs=placed, out_specs=placed, check_vma=False)
```

```python
import functools

import jax
import jax.numpy as jnp
from jax import lax
from jax.experimental import pallas as pl
from jax.experimental.pallas import tpu as pltpu
from jax.sharding import PartitionSpec as P

VMEM_BYTES = 67043328
HIGHEST = lax.Precision.HIGHEST


def dot(a, b):
    return jnp.dot(a, b, precision=HIGHEST, preferred_element_type=jnp.float32)


def upper_inverse(matrix):
    order = matrix.shape[0]
    row = lax.broadcasted_iota(jnp.int32, (order, order), 0)
    col = lax.broadcasted_iota(jnp.int32, (order, order), 1)
    on_diag = row == col
    pivots = jnp.where(on_diag, matrix, 0.0)
    recip_col = 1.0 / jnp.sum(pivots, axis=1, keepdims=True)
    recip_row = 1.0 / jnp.sum(pivots, axis=0, keepdims=True)
    power = -(recip_col * jnp.where(col > row, matrix, 0.0))
    identity = jnp.where(on_diag, 1.0, 0.0)
    product = identity + power
    steps = max((order - 1).bit_length(), 1)
    for level in range(steps - 1):
        power = dot(power, power)
        product = dot(product, identity + power)
    return product * recip_row


def split(value):
    high = value.astype(jnp.bfloat16)
    low = (value - high.astype(jnp.float32)).astype(jnp.bfloat16)
    return high, low


def kernel(n_mc, n_mr, chunks, late, tile, detour,
           column_ref, diag_ref, row_ref, trailing_ref,
           solved_ref, inverse_ref, scaled_ref, updated_ref, panel, left_high, left_low,
           columns, diags, matrix, flipped, carried,
           load_sem, trail_sem, send_sem, line_recv, half_recv, pair_recv, rest_recv,
           diag_send, diag_recv, block_send, block_recv, col_send, col_recv, own_send, carry_send, carry_recv):
    mc = lax.axis_index("mc")
    mr = lax.axis_index("mr")
    levels = n_mc // 2
    z = mc // 2
    x = lax.rem(mc, 2)
    rows = row_ref.shape[0]
    half = rows // 2
    cols = row_ref.shape[1]
    width = cols // chunks
    block_cols = diag_ref.shape[1]
    height = column_ref.shape[1]
    last = levels - 1
    final = chunks - 1
    kept = width - detour
    per = block_cols // (2 * rows) if block_cols % (2 * rows) == 0 else levels
    needed = lambda m: jnp.minimum(levels, (m + 1) * per)
    limit = needed(mr)

    def at(mc_index, mr_index):
        return {"mc": mc_index, "mr": mr_index}

    down = jnp.maximum(mc - 2, 0)
    up = jnp.minimum(mc + 2, n_mc - 1)
    across = z * 2 + 1 - x
    other = 1 - x
    top = 2 * last + other
    bottom = other

    barrier = pltpu.get_barrier_semaphore()

    def greet(mc_index, mr_index):
        pl.semaphore_signal(barrier, inc=1, device_id=at(mc_index, mr_index),
                            device_id_type=pl.DeviceIdType.MESH)

    @pl.when(z > 0)
    def _():
        greet(down, mr)

    @pl.when(z < last)
    def _():
        greet(up, mr)

    greet(across, mr)
    for step in range(1, n_mr):
        greet(mc, lax.rem(mr + step, n_mr))

    own_rows = pl.ds(pl.multiple_of(mc * rows, rows), rows)
    own_part = lambda k: pl.ds(pl.multiple_of(k * block_cols, block_cols), block_cols)
    own_diag = pltpu.make_async_copy(diag_ref, diags.at[mr, own_rows], load_sem.at[0])
    own_column = pltpu.make_async_copy(column_ref, columns.at[own_part(mr)], load_sem.at[1])
    own_first = pltpu.make_async_copy(
        row_ref.at[:, pl.ds(0, width)], panel.at[own_rows, pl.ds(0, width)], load_sem.at[2])
    own_diag.start()
    own_first.start()
    if chunks > 1:
        own_rest = pltpu.make_async_copy(
            row_ref.at[:, pl.ds(width, cols - width)], panel.at[own_rows, pl.ds(width, cols - width)],
            load_sem.at[3])
        own_rest.start()
    own_column.start()
    pl.semaphore_wait(barrier, n_mr + jnp.where(z > 0, 1, 0) + jnp.where(z < last, 1, 0))

    def remote(ref, send, recv, mc_index, mr_index):
        return pltpu.make_async_remote_copy(
            src_ref=ref, dst_ref=ref, send_sem=send, recv_sem=recv,
            device_id=at(mc_index, mr_index), device_id_type=pl.DeviceIdType.MESH)

    def piece(shard, c, low=None, span=None):
        first = pl.multiple_of(shard * rows, rows)
        count = rows
        if low is not None:
            first = pl.multiple_of(shard * rows + low * half, half)
            count = half
        return panel.at[pl.ds(first, count), pl.ds(pl.multiple_of(c * width, width), span or width)]

    target = (down, up, across)

    def line(q, c, way, send=None, span=None):
        return remote(piece(2 * q + x, c, None, span), send_sem.at[way] if send is None else send,
                      line_recv.at[q, c], target[way], mr)

    def split_piece(c, way):
        return remote(piece((top, bottom)[way], c, 1), send_sem.at[way], half_recv.at[way, c], target[way], mr)

    def pair(shard, c, send=None, span=None):
        return remote(piece(shard, c, None, span), send_sem.at[2] if send is None else send,
                      pair_recv.at[c], across, mr)

    def cross(q, c, low=None):
        return remote(piece(2 * q + x, c, low), send_sem.at[2], rest_recv.at[c], across, mr)

    def diag_line(q, way):
        ref = diags.at[mr, pl.ds(pl.multiple_of((2 * q + x) * rows, rows), rows)]
        return remote(ref, diag_send.at[way], diag_recv.at[q if way < 2 else levels], target[way], mr)

    def block_copy(k, step):
        return remote(diags.at[k], block_send.at[0], block_recv.at[0], mc, lax.rem(mr + step, n_mr))

    def column_copy(k, step):
        return remote(columns.at[own_part(k)], col_send.at[0], col_recv.at[0], mc, lax.rem(mr + step, n_mr))

    def send_row(c):
        def send(span):
            send = own_send.at[0] if c == final else None

            @pl.when(z > 0)
            def _():
                line(z, c, 0, send, span).start()

            @pl.when(z < last)
            def _():
                line(z, c, 1, send, span).start()

            pair(mc, c, send, span).start()

        if c == final and detour:
            by_mr(lambda: send(kept), lambda: send(width))
        else:
            send(width)

    def by_mr(first, others):
        pl.when(mr == 0)(first)
        pl.when(mr != 0)(others)

    sides = (z > 0, z < last, None)

    def each_side(act):
        for way in range(3):
            if sides[way] is None:
                act(way)
            else:
                pl.when(sides[way])(functools.partial(act, way))

    def detoured(shard):
        return panel.at[pl.ds(pl.multiple_of(shard * rows, rows), rows), pl.ds(final * width + kept, detour)]

    def carry_out():
        return pltpu.make_async_remote_copy(
            src_ref=detoured(mc), dst_ref=carried.at[0], send_sem=carry_send.at[0], recv_sem=carry_recv.at[0],
            device_id=at(mc, n_mr - 1), device_id_type=pl.DeviceIdType.MESH)

    def carry_on(way):
        return pltpu.make_async_remote_copy(
            src_ref=carried.at[0], dst_ref=carried.at[1 + way], send_sem=carry_send.at[0],
            recv_sem=carry_recv.at[1 + way], device_id=at(target[way], mr), device_id_type=pl.DeviceIdType.MESH)

    def carry_home(way):
        shard = (mc + 2, mc - 2, across)[way]
        return pltpu.make_async_remote_copy(
            src_ref=carried.at[1 + way], dst_ref=detoured(shard), send_sem=carry_send.at[1],
            recv_sem=carry_recv.at[1 + way], device_id=at(mc, 0), device_id_type=pl.DeviceIdType.MESH)

    sources = (z < last, z > 0, None)

    def each_source(act):
        for way in range(3):
            if sources[way] is None:
                act(way)
            else:
                pl.when(sources[way])(functools.partial(act, way))

    own_diag.wait()

    @pl.when(z < limit)
    def _():
        each_side(lambda way: diag_line(z, way).start())

    own_first.wait()
    send_row(0)
    if chunks > 1:
        own_rest.wait()
    if detour:
        @pl.when(mr == 0)
        def _():
            carry_out().start()
    own_column.wait()
    for step in range(1, n_mr):
        column_copy(mr, step).start()
    load_trailing = pltpu.make_async_copy(trailing_ref, updated_ref, trail_sem.at[0])
    load_trailing.start()

    for hop in range(last):
        above = z + 1 + hop
        below = z - 1 - hop

        @pl.when(above < limit)
        def _():
            diag_line(above, 0).wait_recv()

            @pl.when(z > 0)
            def _():
                diag_line(above, 0).start()

            diag_line(above, 2).start()

        @pl.when(jnp.logical_and(below >= 0, below < limit))
        def _():
            diag_line(below, 1).wait_recv()

            @pl.when(z < last)
            def _():
                diag_line(below, 1).start()

            diag_line(below, 2).start()

        if hop == 0 and detour:
            @pl.when(mr == n_mr - 1)
            def _():
                carry_out().wait_recv()
                each_side(lambda way: carry_on(way).start())
        if hop + 1 < chunks:
            send_row(hop + 1)
    for c in range(levels, chunks):
        send_row(c)
    if detour:
        @pl.when(mr == n_mr - 1)
        def _():
            def pass_home(way):
                carry_on(way).wait_recv()
                carry_home(way).start()

            each_source(pass_home)

    first_half_only = lambda q: jnp.logical_or(
        jnp.logical_and(q == last, z != last), jnp.logical_and(q == 0, z != 0))

    def send_across(q, c):
        @pl.when(first_half_only(q))
        def _():
            cross(q, c, 0).start()

        @pl.when(jnp.logical_not(first_half_only(q)))
        def _():
            cross(q, c).start()

    def invert():
        for m in range(n_mr):
            @pl.when(mr == m)
            def _():
                ref = diags.at[m, pl.ds(0, min(levels, (m + 1) * per) * rows)]
                remote(ref, diag_send.at[2], diag_recv.at[levels], across, mr).wait_recv()
        for step in range(1, n_mr):
            block_copy(mr, step).start()
        remote(diags.at[pl.ds(0, n_mr - 1)], block_send.at[0], block_recv.at[0], mc, lax.rem(mr + 1, n_mr)).wait_recv()
        for k in range(n_mr):
            matrix[:, k * block_cols:(k + 1) * block_cols] = diags[k]
        matrix[...] = upper_inverse(matrix[...])
        own_inverse = matrix[own_rows, :]
        remote(columns.at[pl.ds(0, (n_mr - 1) * block_cols)], col_send.at[0], col_recv.at[0], mc,
               lax.rem(mr + 1, n_mr)).wait_recv()
        flipped[...] = -lax.dot_general(
            matrix[...], columns[...], (((0,), (0,)), ((), ())),
            precision=HIGHEST, preferred_element_type=jnp.float32)
        solved_ref[...] = flipped[own_part(mr), :]
        left_high[0:height, :], left_low[0:height, :] = split(flipped[...].T)
        left_high[height:height + rows, :], left_low[height:height + rows, :] = split(own_inverse)
        for k in range(n_mr):
            @pl.when(mr == k)
            def _():
                inverse_ref[...] = own_inverse[:, k * block_cols:(k + 1) * block_cols]

    for phase in range(last):
        if phase == min(1, levels - 2):
            invert()

        above = z + 1 + phase
        below = z - 1 - phase

        def step(c, arrive):
            @pl.when(above < levels)
            def _():
                arrive(0, lambda span: line(above, c, 0, None, span))

                @pl.when(z > 0)
                def _():
                    line(above, c, 0).start()

                send_across(above, c)

            @pl.when(below >= 0)
            def _():
                arrive(1, lambda span: line(below, c, 1, None, span))

                @pl.when(z < last)
                def _():
                    line(below, c, 1).start()

                send_across(below, c)

            if phase == 0:
                arrive(2, lambda span: pair(2 * z + other, c, None, span))

                @pl.when(z == last)
                def _():
                    split_piece(c, 0).start()

                @pl.when(z == 0)
                def _():
                    split_piece(c, 1).start()

            @pl.when(above == levels)
            def _():
                @pl.when(z < last)
                def _():
                    split_piece(c, 0).wait_recv()

                    @pl.when(z > 0)
                    def _():
                        split_piece(c, 0).start()

            @pl.when(below == -1)
            def _():
                @pl.when(z > 0)
                def _():
                    split_piece(c, 1).wait_recv()

                    @pl.when(z < last)
                    def _():
                        split_piece(c, 1).start()

        def whole(way, make):
            make(width).wait_recv()

        def joined(way, make):
            def first():
                make(kept).wait_recv()
                carry_home(way).wait_recv()

            by_mr(first, lambda: make(width).wait_recv())

        split_last = phase == 0 and detour > 0
        pl.loop(0, chunks - 1 if split_last else chunks)(lambda c: step(c, whole))
        if split_last:
            step(final, joined)

    def receive_rest(c):
        @pl.when(z == 0)
        def _():
            split_piece(c, 0).wait_recv()

        @pl.when(z == last)
        def _():
            split_piece(c, 1).wait_recv()

        def gathered(halves):
            ref = panel.at[pl.ds(0, halves * half), pl.ds(0, width)]
            remote(ref, send_sem.at[2], rest_recv.at[c], across, mr).wait_recv()

        at_end = jnp.logical_or(z == 0, z == last)

        @pl.when(at_end)
        def _():
            gathered(2 * levels - 3)

        if levels > 2:
            @pl.when(jnp.logical_not(at_end))
            def _():
                gathered(2 * levels - 4)

    load_trailing.wait()

    @pl.loop(0, chunks - late)
    def _(c):
        receive_rest(c)
        for t in range(width // tile):
            part = pl.ds(pl.multiple_of(c * width + t * tile, tile), tile)
            product = multiply(left_high, left_low, panel[:, part])
            updated_ref[:, part] = updated_ref[:, part] + product[0:height]
            scaled_ref[:, part] = product[height:height + rows]

    for c in range(chunks - late, chunks):
        receive_rest(c)

    def sent(way, halves):
        ref = panel.at[pl.ds(0, halves * half - rows // chunks)]
        remote(ref, send_sem.at[way], pair_recv.at[0], target[way], mr).wait_send()

    def sent_own(count, span):
        ref = panel.at[pl.ds(0, count * rows), pl.ds(0, span)]
        remote(ref, own_send.at[0], pair_recv.at[0], across, mr).wait_send()

    def sent_diag(way, count):
        if count > 0:
            ref = diags.at[mr, pl.ds(0, count * rows)]
            remote(ref, diag_send.at[way], diag_recv.at[0], target[way], mr).wait_send()

    def sent_carry(slot, count):
        remote(carried.at[pl.ds(0, count)], carry_send.at[slot], carry_recv.at[0], across, mr).wait_send()

    for k in range(levels):
        @pl.when(z == k)
        def _():
            count = 1 + (k > 0) + (k < last)
            if k > 0:
                sent(0, 2 * (levels - k) + 1)
            if k < last:
                sent(1, 2 * (k + 1) + 1)
            sent(2, 2 * levels - (1 if k in (0, last) else 2))
            if detour:
                by_mr(lambda: sent_own(count, kept), lambda: sent_own(count, width))

                @pl.when(mr == n_mr - 1)
                def _():
                    sent_carry(0, count)
                    sent_carry(1, count)
            else:
                sent_own(count, width)
            for m in range(n_mr):
                @pl.when(mr == m)
                def _():
                    most = min(levels, (m + 1) * per)
                    if k > 0:
                        sent_diag(0, most - k)
                    if k < last:
                        sent_diag(1, min(k + 1, most))
                    sent_diag(2, most)

    if detour:
        @pl.when(mr == 0)
        def _():
            sent_carry(0, 1)

    remote(diags.at[pl.ds(0, n_mr - 1)], block_send.at[0], block_recv.at[0], mc, lax.rem(mr + 1, n_mr)).wait_send()
    remote(columns.at[pl.ds(0, (n_mr - 1) * block_cols)], col_send.at[0], col_recv.at[0], mc,
           lax.rem(mr + 1, n_mr)).wait_send()


def multiply(left_high, left_low, right):
    right_high, right_low = split(right)
    product = jnp.dot(left_high[...], right_low, preferred_element_type=jnp.float32)
    product += jnp.dot(left_low[...], right_high, preferred_element_type=jnp.float32)
    return product + jnp.dot(left_high[...], right_high, preferred_element_type=jnp.float32)


def finish(done, tile, solved, inverse, scaled, updated, panel, left_high, left_low,
           solved_out, inverse_out, scaled_out, updated_out, held_updated, held_scaled, sem, tile_sem):
    height, cols = updated.shape
    strips = sem.shape[0] - 3
    deep = height // strips
    ready = pl.ds(0, done)
    copies = []
    for i in range(strips):
        part = pl.ds(i * deep, deep)
        copies.append(pltpu.make_async_copy(updated.at[part, ready], updated_out.at[part, ready], sem.at[3 + i]))
    copies.append(pltpu.make_async_copy(solved, solved_out, sem.at[0]))
    copies.append(pltpu.make_async_copy(inverse, inverse_out, sem.at[1]))
    copies.append(pltpu.make_async_copy(scaled.at[:, ready], scaled_out.at[:, ready], sem.at[2]))
    for c in copies:
        c.start()
    for t in range((cols - done) // tile):
        part = pl.ds(done + t * tile, tile)
        slot = pl.ds(t * tile, tile)
        product = multiply(left_high, left_low, panel[:, part])
        held_updated[:, slot] = updated[:, part] + product[0:height]
        held_scaled[:, slot] = product[height:]
        copies.append(pltpu.make_async_copy(held_updated.at[:, slot], updated_out.at[:, part], tile_sem.at[0, t]))
        copies.append(pltpu.make_async_copy(held_scaled.at[:, slot], scaled_out.at[:, part], tile_sem.at[1, t]))
        copies[-2].start()
        copies[-1].start()
    for c in copies:
        c.wait()


def shards(n_mc, n_mr, column_panel, diag_block, row_panel, trailing):
    rows, block_cols = diag_block.shape
    height, cols = trailing.shape
    order = rows * n_mc
    levels = n_mc // 2
    chunks = max(1, 16 // levels)
    while cols % (chunks * 128):
        chunks //= 2
    late = 1 if chunks > 1 else 0
    width = cols // chunks
    done = cols - late * width
    tile = 512 if width % 512 == 0 else 128
    detour = 3 * width // 2048 * 128 if n_mr > 1 and chunks > 1 and levels > 1 else 0
    held = 4 * (height * cols + rows * cols + block_cols * height + rows * 128 + order * cols
                + (height + rows) * order) + 64 * 1024
    dma = pltpu.SemaphoreType.DMA
    f32 = jnp.float32
    anywhere = pl.BlockSpec(memory_space=pl.ANY)
    vmem = pl.BlockSpec(memory_space=pltpu.VMEM)
    parts = pl.pallas_call(
        functools.partial(kernel, n_mc, n_mr, chunks, late, tile, detour),
        out_shape=(
            pltpu.VMEM((block_cols, height), f32),
            pltpu.VMEM(diag_block.shape, f32),
            pltpu.VMEM(row_panel.shape, f32),
            pltpu.VMEM(trailing.shape, f32),
            pltpu.VMEM((order, cols), f32),
            pltpu.VMEM((height + rows, order), jnp.bfloat16),
            pltpu.VMEM((height + rows, order), jnp.bfloat16),
        ),
        in_specs=[pl.BlockSpec(memory_space=pltpu.HBM)] * 4,
        out_specs=(vmem,) * 7,
        scratch_shapes=[
            pltpu.VMEM((order, height), f32),
            pltpu.VMEM((n_mr, order, block_cols), f32),
            pltpu.VMEM((order, order), f32),
            pltpu.VMEM((order, height), f32),
            pltpu.VMEM((4, rows, max(detour, 128)), f32),
            dma((4,)), dma((1,)), dma((3,)), dma((levels, chunks)), dma((2, chunks)), dma((chunks,)), dma((chunks,)),
            dma((3,)), dma((levels + 1,)), dma((1,)), dma((1,)), dma((1,)), dma((1,)),
            dma((1,)), dma((2,)), dma((4,)),
        ],
        compiler_params=pltpu.CompilerParams(
            collective_id=0, has_side_effects=True, vmem_limit_bytes=VMEM_BYTES - held),
    )(column_panel.T, diag_block, row_panel, trailing)
    tiles = max(1, (cols - done) // tile)
    spare = max(tile, cols - done)
    solved, inverse, scaled, updated = pl.pallas_call(
        functools.partial(finish, done, tile),
        out_shape=tuple(jax.ShapeDtypeStruct(part.shape, f32) for part in parts[:4]),
        in_specs=[vmem] * 7,
        out_specs=(anywhere,) * 4,
        scratch_shapes=[pltpu.VMEM((height, spare), f32), pltpu.VMEM((rows, spare), f32), dma((3 + 8,)),
                        dma((2, tiles))],
        compiler_params=pltpu.CompilerParams(vmem_limit_bytes=4 * (height + rows) * (spare + 4 * tile) + 1024 * 1024),
    )(*parts)
    return solved.T, inverse, scaled, updated


def solution(mesh):
    placed = (P("mc", "mr"),) * 4
    return jax.shard_map(
        functools.partial(shards, mesh.shape["mc"], mesh.shape["mr"]),
        mesh=mesh, in_specs=placed, out_specs=placed, check_vma=False)
```

```python
import functools

import jax
import jax.numpy as jnp
from jax import lax
from jax.experimental import pallas as pl
from jax.experimental.pallas import tpu as pltpu
from jax.sharding import PartitionSpec as P

VMEM_BYTES = 67043328
HIGHEST = lax.Precision.HIGHEST


def dot(a, b):
    return jnp.dot(a, b, precision=HIGHEST, preferred_element_type=jnp.float32)


def upper_inverse(matrix):
    order = matrix.shape[0]
    row = lax.broadcasted_iota(jnp.int32, (order, order), 0)
    col = lax.broadcasted_iota(jnp.int32, (order, order), 1)
    on_diag = row == col
    pivots = jnp.where(on_diag, matrix, 0.0)
    recip_col = 1.0 / jnp.sum(pivots, axis=1, keepdims=True)
    recip_row = 1.0 / jnp.sum(pivots, axis=0, keepdims=True)
    power = -(recip_col * jnp.where(col > row, matrix, 0.0))
    identity = jnp.where(on_diag, 1.0, 0.0)
    product = identity + power
    steps = max((order - 1).bit_length(), 1)
    for level in range(steps - 1):
        power = dot(power, power)
        product = dot(product, identity + power)
    return product * recip_row


def split(value):
    high = value.astype(jnp.bfloat16)
    low = (value - high.astype(jnp.float32)).astype(jnp.bfloat16)
    return high, low


def kernel(n_mc, n_mr, chunks, late, tile, detour,
           column_ref, diag_ref, row_ref, trailing_ref,
           solved_ref, inverse_ref, scaled_ref, updated_ref, panel, left_high, left_low,
           columns, diags, matrix, flipped, carried,
           load_sem, trail_sem, send_sem, line_recv, half_recv, pair_recv, rest_recv,
           diag_send, diag_recv, block_send, block_recv, col_send, col_recv, own_send, carry_send, carry_recv,
           ready_sem):
    mc = lax.axis_index("mc")
    mr = lax.axis_index("mr")
    levels = n_mc // 2
    z = mc // 2
    x = lax.rem(mc, 2)
    rows = row_ref.shape[0]
    half = rows // 2
    cols = row_ref.shape[1]
    width = cols // chunks
    block_cols = diag_ref.shape[1]
    height = column_ref.shape[1]
    last = levels - 1
    final = chunks - 1
    kept = width - detour
    per = block_cols // (2 * rows) if block_cols % (2 * rows) == 0 else levels
    needed = lambda m: jnp.minimum(levels, (m + 1) * per)
    limit = needed(mr)

    def at(mc_index, mr_index):
        return {"mc": mc_index, "mr": mr_index}

    down = jnp.maximum(mc - 2, 0)
    up = jnp.minimum(mc + 2, n_mc - 1)
    across = z * 2 + 1 - x
    other = 1 - x
    top = 2 * last + other
    bottom = other

    barrier = pltpu.get_barrier_semaphore()

    def greet(mc_index, mr_index):
        pl.semaphore_signal(barrier, inc=1, device_id=at(mc_index, mr_index),
                            device_id_type=pl.DeviceIdType.MESH)

    @pl.when(z > 0)
    def _():
        greet(down, mr)

    @pl.when(z < last)
    def _():
        greet(up, mr)

    greet(across, mr)
    twins = n_mr // 2 - 1 if n_mr % 2 == 0 else 0
    if n_mr % 2 == 0:
        greet(mc, mr + 1 - 2 * lax.rem(mr, 2))
        for step in range(2, n_mr, 2):
            greet(mc, lax.rem(mr + step, n_mr))
    else:
        for step in range(1, n_mr):
            greet(mc, lax.rem(mr + step, n_mr))
    greeted = 2 + twins if n_mr % 2 == 0 else n_mr

    own_rows = pl.ds(pl.multiple_of(mc * rows, rows), rows)
    own_part = lambda k: pl.ds(pl.multiple_of(k * block_cols, block_cols), block_cols)
    own_diag = pltpu.make_async_copy(diag_ref, diags.at[mr, own_rows], load_sem.at[0])
    own_column = pltpu.make_async_copy(column_ref, columns.at[own_part(mr)], load_sem.at[1])
    own_first = pltpu.make_async_copy(
        row_ref.at[:, pl.ds(0, width)], panel.at[own_rows, pl.ds(0, width)], load_sem.at[2])
    own_diag.start()
    own_first.start()
    if chunks > 1:
        own_rest = pltpu.make_async_copy(
            row_ref.at[:, pl.ds(width, cols - width)], panel.at[own_rows, pl.ds(width, cols - width)],
            load_sem.at[3])
        own_rest.start()
    own_column.start()
    pl.semaphore_wait(barrier, greeted + jnp.where(z > 0, 1, 0) + jnp.where(z < last, 1, 0))

    def remote(ref, send, recv, mc_index, mr_index):
        return pltpu.make_async_remote_copy(
            src_ref=ref, dst_ref=ref, send_sem=send, recv_sem=recv,
            device_id=at(mc_index, mr_index), device_id_type=pl.DeviceIdType.MESH)

    def piece(shard, c, low=None, span=None):
        first = pl.multiple_of(shard * rows, rows)
        count = rows
        if low is not None:
            first = pl.multiple_of(shard * rows + low * half, half)
            count = half
        return panel.at[pl.ds(first, count), pl.ds(pl.multiple_of(c * width, width), span or width)]

    target = (down, up, across)

    def line(q, c, way, send=None, span=None):
        return remote(piece(2 * q + x, c, None, span), send_sem.at[way] if send is None else send,
                      line_recv.at[q - 1 if way == 0 else q, c], target[way], mr)

    def split_piece(c, way):
        return remote(piece((top, bottom)[way], c, 1), send_sem.at[way], half_recv.at[way, c], target[way], mr)

    def pair(shard, c, send=None, span=None):
        return remote(piece(shard, c, None, span), send_sem.at[2] if send is None else send,
                      pair_recv.at[c], across, mr)

    def cross(q, c, low=None):
        return remote(piece(2 * q + x, c, low), send_sem.at[2], rest_recv.at[c], across, mr)

    def diag_line(q, way):
        ref = diags.at[mr, pl.ds(pl.multiple_of((2 * q + x) * rows, rows), rows)]
        return remote(ref, diag_send.at[way], diag_recv.at[q if way < 2 else levels], target[way], mr)

    def block_copy(k, step):
        return remote(diags.at[k], block_send.at[0], block_recv.at[0], mc, lax.rem(mr + step, n_mr))

    def column_copy(k, step):
        return remote(columns.at[own_part(k)], col_send.at[0], col_recv.at[0], mc, lax.rem(mr + step, n_mr))

    def send_row(c):
        def send(span):
            send = own_send.at[0] if c == final else None

            @pl.when(z > 0)
            def _():
                line(z, c, 0, send, span).start()

            @pl.when(z < last)
            def _():
                line(z, c, 1, send, span).start()

            pair(mc, c, send, span).start()

        if c == final and detour:
            by_mr(lambda: send(kept), lambda: send(width))
        else:
            send(width)

    def by_mr(first, others):
        pl.when(mr == 0)(first)
        pl.when(mr != 0)(others)

    sides = (z > 0, z < last, None)

    def each_side(act):
        for way in range(3):
            if sides[way] is None:
                act(way)
            else:
                pl.when(sides[way])(functools.partial(act, way))

    def detoured(shard):
        return panel.at[pl.ds(pl.multiple_of(shard * rows, rows), rows), pl.ds(final * width + kept, detour)]

    def carry_out():
        return pltpu.make_async_remote_copy(
            src_ref=detoured(mc), dst_ref=carried.at[0], send_sem=carry_send.at[0], recv_sem=carry_recv.at[0],
            device_id=at(mc, n_mr - 1), device_id_type=pl.DeviceIdType.MESH)

    def carry_on(way):
        return pltpu.make_async_remote_copy(
            src_ref=carried.at[0], dst_ref=carried.at[1 + way], send_sem=carry_send.at[0],
            recv_sem=carry_recv.at[1 + way], device_id=at(target[way], mr), device_id_type=pl.DeviceIdType.MESH)

    def carry_home(way):
        shard = (mc + 2, mc - 2, across)[way]
        return pltpu.make_async_remote_copy(
            src_ref=carried.at[1 + way], dst_ref=detoured(shard), send_sem=carry_send.at[1],
            recv_sem=carry_recv.at[1 + way], device_id=at(mc, 0), device_id_type=pl.DeviceIdType.MESH)

    sources = (z < last, z > 0, None)

    def each_source(act):
        for way in range(3):
            if sources[way] is None:
                act(way)
            else:
                pl.when(sources[way])(functools.partial(act, way))

    own_diag.wait()

    @pl.when(z < limit)
    def _():
        each_side(lambda way: diag_line(z, way).start())

    own_first.wait()
    send_row(0)
    if twins:
        for step in range(2, n_mr, 2):
            pl.semaphore_signal(ready_sem.at[0], inc=1, device_id=at(mc, lax.rem(mr + step, n_mr)),
                                device_id_type=pl.DeviceIdType.MESH)
    if chunks > 1:
        own_rest.wait()
    if twins:
        pl.semaphore_wait(ready_sem.at[0], twins)
    if detour:
        @pl.when(mr == 0)
        def _():
            carry_out().start()
    own_column.wait()
    for step in range(1, n_mr):
        column_copy(mr, step).start()
    load_trailing = pltpu.make_async_copy(trailing_ref, updated_ref, trail_sem.at[0])
    load_trailing.start()

    for hop in range(last):
        above = z + 1 + hop
        below = z - 1 - hop

        @pl.when(above < limit)
        def _():
            diag_line(above, 0).wait_recv()

            @pl.when(z > 0)
            def _():
                diag_line(above, 0).start()

            diag_line(above, 2).start()

        @pl.when(jnp.logical_and(below >= 0, below < limit))
        def _():
            diag_line(below, 1).wait_recv()

            @pl.when(z < last)
            def _():
                diag_line(below, 1).start()

            diag_line(below, 2).start()

        if hop == 0 and detour:
            @pl.when(mr == n_mr - 1)
            def _():
                carry_out().wait_recv()
                each_side(lambda way: carry_on(way).start())
        if hop + 1 < chunks:
            send_row(hop + 1)
    for c in range(levels, chunks):
        send_row(c)
    if detour:
        @pl.when(mr == n_mr - 1)
        def _():
            def pass_home(way):
                carry_on(way).wait_recv()
                carry_home(way).start()

            each_source(pass_home)

    first_half_only = lambda q: jnp.logical_or(
        jnp.logical_and(q == last, z != last), jnp.logical_and(q == 0, z != 0))

    def send_across(q, c):
        @pl.when(first_half_only(q))
        def _():
            cross(q, c, 0).start()

        @pl.when(jnp.logical_not(first_half_only(q)))
        def _():
            cross(q, c).start()

    def invert():
        for m in range(n_mr):
            @pl.when(mr == m)
            def _():
                ref = diags.at[m, pl.ds(0, min(levels, (m + 1) * per) * rows)]
                remote(ref, diag_send.at[2], diag_recv.at[levels], across, mr).wait_recv()
        for step in range(1, n_mr):
            block_copy(mr, step).start()
        remote(diags.at[pl.ds(0, n_mr - 1)], block_send.at[0], block_recv.at[0], mc, lax.rem(mr + 1, n_mr)).wait_recv()
        for k in range(n_mr):
            matrix[:, k * block_cols:(k + 1) * block_cols] = diags[k]
        matrix[...] = upper_inverse(matrix[...])
        own_inverse = matrix[own_rows, :]
        remote(columns.at[pl.ds(0, (n_mr - 1) * block_cols)], col_send.at[0], col_recv.at[0], mc,
               lax.rem(mr + 1, n_mr)).wait_recv()
        flipped[...] = -lax.dot_general(
            matrix[...], columns[...], (((0,), (0,)), ((), ())),
            precision=HIGHEST, preferred_element_type=jnp.float32)
        solved_ref[...] = flipped[own_part(mr), :]
        left_high[0:height, :], left_low[0:height, :] = split(flipped[...].T)
        left_high[height:height + rows, :], left_low[height:height + rows, :] = split(own_inverse)
        for k in range(n_mr):
            @pl.when(mr == k)
            def _():
                inverse_ref[...] = own_inverse[:, k * block_cols:(k + 1) * block_cols]

    for phase in range(last):
        if phase == min(1, levels - 2):
            invert()

        above = z + 1 + phase
        below = z - 1 - phase

        def step(c, arrive):
            @pl.when(above < levels)
            def _():
                arrive(0, lambda span: line(above, c, 0, None, span))

                @pl.when(z > 0)
                def _():
                    line(above, c, 0).start()

                send_across(above, c)

            @pl.when(below >= 0)
            def _():
                arrive(1, lambda span: line(below, c, 1, None, span))

                @pl.when(z < last)
                def _():
                    line(below, c, 1).start()

                send_across(below, c)

            if phase == 0:
                arrive(2, lambda span: pair(2 * z + other, c, None, span))

                @pl.when(z == last)
                def _():
                    split_piece(c, 0).start()

                @pl.when(z == 0)
                def _():
                    split_piece(c, 1).start()

            @pl.when(above == levels)
            def _():
                @pl.when(z < last)
                def _():
                    split_piece(c, 0).wait_recv()

                    @pl.when(z > 0)
                    def _():
                        split_piece(c, 0).start()

            @pl.when(below == -1)
            def _():
                @pl.when(z > 0)
                def _():
                    split_piece(c, 1).wait_recv()

                    @pl.when(z < last)
                    def _():
                        split_piece(c, 1).start()

        def whole(way, make):
            make(width).wait_recv()

        def joined(way, make):
            def first():
                make(kept).wait_recv()
                carry_home(way).wait_recv()

            by_mr(first, lambda: make(width).wait_recv())

        split_last = phase == 0 and detour > 0
        pl.loop(0, chunks - 1 if split_last else chunks)(lambda c: step(c, whole))
        if split_last:
            step(final, joined)

    def receive_rest(c):
        @pl.when(z == 0)
        def _():
            split_piece(c, 0).wait_recv()

        @pl.when(z == last)
        def _():
            split_piece(c, 1).wait_recv()

        def gathered(halves):
            ref = panel.at[pl.ds(0, halves * half), pl.ds(0, width)]
            remote(ref, send_sem.at[2], rest_recv.at[c], across, mr).wait_recv()

        at_end = jnp.logical_or(z == 0, z == last)

        @pl.when(at_end)
        def _():
            gathered(2 * levels - 3)

        if levels > 2:
            @pl.when(jnp.logical_not(at_end))
            def _():
                gathered(2 * levels - 4)

    load_trailing.wait()

    @pl.loop(0, chunks - late)
    def _(c):
        receive_rest(c)
        for t in range(width // tile):
            part = pl.ds(pl.multiple_of(c * width + t * tile, tile), tile)
            product = multiply(left_high, left_low, panel[:, part])
            updated_ref[:, part] = updated_ref[:, part] + product[0:height]
            scaled_ref[:, part] = product[height:height + rows]

    for c in range(chunks - late, chunks):
        receive_rest(c)

    def sent(way, halves):
        ref = panel.at[pl.ds(0, halves * half - rows // chunks)]
        remote(ref, send_sem.at[way], pair_recv.at[0], target[way], mr).wait_send()

    def sent_own(count, span):
        ref = panel.at[pl.ds(0, count * rows), pl.ds(0, span)]
        remote(ref, own_send.at[0], pair_recv.at[0], across, mr).wait_send()

    def sent_diag(way, count):
        if count > 0:
            ref = diags.at[mr, pl.ds(0, count * rows)]
            remote(ref, diag_send.at[way], diag_recv.at[0], target[way], mr).wait_send()

    def sent_carry(slot, count):
        remote(carried.at[pl.ds(0, count)], carry_send.at[slot], carry_recv.at[0], across, mr).wait_send()

    for k in range(levels):
        @pl.when(z == k)
        def _():
            count = 1 + (k > 0) + (k < last)
            if k > 0:
                sent(0, 2 * (levels - k) + 1)
            if k < last:
                sent(1, 2 * (k + 1) + 1)
            sent(2, 2 * levels - (1 if k in (0, last) else 2))
            if detour:
                by_mr(lambda: sent_own(count, kept), lambda: sent_own(count, width))

                @pl.when(mr == n_mr - 1)
                def _():
                    sent_carry(0, count)
                    sent_carry(1, count)
            else:
                sent_own(count, width)
            for m in range(n_mr):
                @pl.when(mr == m)
                def _():
                    most = min(levels, (m + 1) * per)
                    if k > 0:
                        sent_diag(0, most - k)
                    if k < last:
                        sent_diag(1, min(k + 1, most))
                    sent_diag(2, most)

    if detour:
        @pl.when(mr == 0)
        def _():
            sent_carry(0, 1)

    remote(diags.at[pl.ds(0, n_mr - 1)], block_send.at[0], block_recv.at[0], mc, lax.rem(mr + 1, n_mr)).wait_send()
    remote(columns.at[pl.ds(0, (n_mr - 1) * block_cols)], col_send.at[0], col_recv.at[0], mc,
           lax.rem(mr + 1, n_mr)).wait_send()


def multiply(left_high, left_low, right):
    right_high, right_low = split(right)
    product = jnp.dot(left_high[...], right_low, preferred_element_type=jnp.float32)
    product += jnp.dot(left_low[...], right_high, preferred_element_type=jnp.float32)
    return product + jnp.dot(left_high[...], right_high, preferred_element_type=jnp.float32)


def finish(done, tile, solved, inverse, scaled, updated, panel, left_high, left_low,
           solved_out, inverse_out, scaled_out, updated_out, held_updated, held_scaled, sem):
    height, cols = updated.shape
    strips = 8
    deep = height // strips
    ready = pl.ds(0, done)
    rest = pl.ds(done, cols - done)
    for i in range(strips):
        part = pl.ds(i * deep, deep)
        pltpu.make_async_copy(updated.at[part, ready], updated_out.at[part, ready], sem.at[3]).start()
    copies = [
        pltpu.make_async_copy(solved, solved_out, sem.at[0]),
        pltpu.make_async_copy(inverse, inverse_out, sem.at[1]),
        pltpu.make_async_copy(scaled.at[:, ready], scaled_out.at[:, ready], sem.at[2]),
    ]
    for c in copies:
        c.start()
    copies.append(pltpu.make_async_copy(updated.at[:, ready], updated_out.at[:, ready], sem.at[3]))
    for t in range((cols - done) // tile):
        part = pl.ds(done + t * tile, tile)
        slot = pl.ds(t * tile, tile)
        product = multiply(left_high, left_low, panel[:, part])
        held_updated[:, slot] = updated[:, part] + product[0:height]
        held_scaled[:, slot] = product[height:]
        pltpu.make_async_copy(held_updated.at[:, slot], updated_out.at[:, part], sem.at[4]).start()
        pltpu.make_async_copy(held_scaled.at[:, slot], scaled_out.at[:, part], sem.at[5]).start()
    if done < cols:
        copies.append(pltpu.make_async_copy(held_updated, updated_out.at[:, rest], sem.at[4]))
        copies.append(pltpu.make_async_copy(held_scaled, scaled_out.at[:, rest], sem.at[5]))
    for c in copies:
        c.wait()


def shards(n_mc, n_mr, column_panel, diag_block, row_panel, trailing):
    rows, block_cols = diag_block.shape
    height, cols = trailing.shape
    order = rows * n_mc
    levels = n_mc // 2
    chunks = max(1, 16 // levels)
    while cols % (chunks * 128):
        chunks //= 2
    late = 1 if chunks > 1 else 0
    width = cols // chunks
    done = cols - late * width
    tile = 512 if width % 512 == 0 else 128
    detour = width // 1024 * 128 if n_mr > 1 and chunks > 1 and levels > 1 else 0
    held = 4 * (height * cols + rows * cols + block_cols * height + rows * 128 + order * cols
                + (height + rows) * order) + 64 * 1024
    dma = pltpu.SemaphoreType.DMA
    f32 = jnp.float32
    anywhere = pl.BlockSpec(memory_space=pl.ANY)
    vmem = pl.BlockSpec(memory_space=pltpu.VMEM)
    parts = pl.pallas_call(
        functools.partial(kernel, n_mc, n_mr, chunks, late, tile, detour),
        out_shape=(
            pltpu.VMEM((block_cols, height), f32),
            pltpu.VMEM(diag_block.shape, f32),
            pltpu.VMEM(row_panel.shape, f32),
            pltpu.VMEM(trailing.shape, f32),
            pltpu.VMEM((order, cols), f32),
            pltpu.VMEM((height + rows, order), jnp.bfloat16),
            pltpu.VMEM((height + rows, order), jnp.bfloat16),
        ),
        in_specs=[pl.BlockSpec(memory_space=pltpu.HBM)] * 4,
        out_specs=(vmem,) * 7,
        scratch_shapes=[
            pltpu.VMEM((order, height), f32),
            pltpu.VMEM((n_mr, order, block_cols), f32),
            pltpu.VMEM((order, order), f32),
            pltpu.VMEM((order, height), f32),
            pltpu.VMEM((4, rows, max(detour, 128)), f32),
            dma((4,)), dma((1,)), dma((3,)), dma((max(1, levels - 1), chunks)), dma((2, chunks)), dma((chunks,)), dma((chunks,)),
            dma((3,)), dma((levels + 1,)), dma((1,)), dma((1,)), dma((1,)), dma((1,)),
            dma((1,)), dma((2,)), dma((4,)), pltpu.SemaphoreType.REGULAR((1,)),
        ],
        compiler_params=pltpu.CompilerParams(
            collective_id=0, has_side_effects=True, vmem_limit_bytes=VMEM_BYTES - held),
    )(column_panel.T, diag_block, row_panel, trailing)
    spare = max(tile, cols - done)
    solved, inverse, scaled, updated = pl.pallas_call(
        functools.partial(finish, done, tile),
        out_shape=tuple(jax.ShapeDtypeStruct(part.shape, f32) for part in parts[:4]),
        in_specs=[vmem] * 7,
        out_specs=(anywhere,) * 4,
        scratch_shapes=[pltpu.VMEM((height, spare), f32), pltpu.VMEM((rows, spare), f32), dma((6,))],
        compiler_params=pltpu.CompilerParams(vmem_limit_bytes=4 * (height + rows) * (spare + 4 * tile) + 1024 * 1024),
    )(*parts)
    return solved.T, inverse, scaled, updated


def solution(mesh):
    placed = (P("mc", "mr"),) * 4
    return jax.shard_map(
        functools.partial(shards, mesh.shape["mc"], mesh.shape["mr"]),
        mesh=mesh, in_specs=placed, out_specs=placed, check_vma=False)
```

```python
import functools

import jax
import jax.numpy as jnp
from jax import lax
from jax.experimental import pallas as pl
from jax.experimental.pallas import tpu as pltpu
from jax.sharding import PartitionSpec as P

VMEM_BYTES = 67043328
HIGHEST = lax.Precision.HIGHEST


def dot(a, b):
    return jnp.dot(a, b, precision=HIGHEST, preferred_element_type=jnp.float32)


def upper_inverse(matrix):
    order = matrix.shape[0]
    row = lax.broadcasted_iota(jnp.int32, (order, order), 0)
    col = lax.broadcasted_iota(jnp.int32, (order, order), 1)
    on_diag = row == col
    pivots = jnp.where(on_diag, matrix, 0.0)
    recip_col = 1.0 / jnp.sum(pivots, axis=1, keepdims=True)
    recip_row = 1.0 / jnp.sum(pivots, axis=0, keepdims=True)
    power = -(recip_col * jnp.where(col > row, matrix, 0.0))
    identity = jnp.where(on_diag, 1.0, 0.0)
    product = identity + power
    steps = max((order - 1).bit_length(), 1)
    for level in range(steps - 1):
        power = dot(power, power)
        product = dot(product, identity + power)
    return product * recip_row


def split(value):
    high = value.astype(jnp.bfloat16)
    low = (value - high.astype(jnp.float32)).astype(jnp.bfloat16)
    return high, low


def kernel(n_mc, n_mr, chunks, late, tile, detour,
           column_ref, diag_ref, row_ref, trailing_ref,
           solved_ref, inverse_ref, scaled_ref, updated_ref, panel, left_high, left_low,
           columns, diags, matrix, flipped, carried,
           load_sem, trail_sem, send_sem, line_recv, half_recv, pair_recv, rest_recv,
           diag_send, diag_recv, block_send, block_recv, col_send, col_recv, own_send, carry_send, carry_recv,
           ready_sem):
    mc = lax.axis_index("mc")
    mr = lax.axis_index("mr")
    levels = n_mc // 2
    z = mc // 2
    x = lax.rem(mc, 2)
    rows = row_ref.shape[0]
    half = rows // 2
    cols = row_ref.shape[1]
    width = cols // chunks
    block_cols = diag_ref.shape[1]
    height = column_ref.shape[1]
    last = levels - 1
    final = chunks - 1
    kept = width - detour
    per = block_cols // (2 * rows) if block_cols % (2 * rows) == 0 else levels
    needed = lambda m: jnp.minimum(levels, (m + 1) * per)
    limit = needed(mr)

    def at(mc_index, mr_index):
        return {"mc": mc_index, "mr": mr_index}

    down = jnp.maximum(mc - 2, 0)
    up = jnp.minimum(mc + 2, n_mc - 1)
    across = z * 2 + 1 - x
    other = 1 - x
    top = 2 * last + other
    bottom = other

    barrier = pltpu.get_barrier_semaphore()

    def greet(mc_index, mr_index):
        pl.semaphore_signal(barrier, inc=1, device_id=at(mc_index, mr_index),
                            device_id_type=pl.DeviceIdType.MESH)

    pairs = n_mr // 2
    y = mr // 2
    core = lax.rem(mr, 2)

    def tell(sem, mc_index, mr_index):
        pl.semaphore_signal(ready_sem.at[sem], inc=1, device_id=at(mc_index, mr_index),
                            device_id_type=pl.DeviceIdType.MESH)

    @pl.when(z < last)
    def _():
        greet(up, mr)

    @pl.when(x == 0)
    def _():
        greet(across, mr)

    greet(mc, mr + 1 - 2 * core)
    for k in range(pairs):
        @pl.when(k > y)
        def _():
            greet(mc, 2 * k + core)

    own_rows = pl.ds(pl.multiple_of(mc * rows, rows), rows)
    own_part = lambda k: pl.ds(pl.multiple_of(k * block_cols, block_cols), block_cols)
    own_diag = pltpu.make_async_copy(diag_ref, diags.at[mr, own_rows], load_sem.at[0])
    own_column = pltpu.make_async_copy(column_ref, columns.at[own_part(mr)], load_sem.at[1])
    own_first = pltpu.make_async_copy(
        row_ref.at[:, pl.ds(0, width)], panel.at[own_rows, pl.ds(0, width)], load_sem.at[2])
    own_diag.start()
    own_first.start()
    if chunks > 1:
        own_rest = pltpu.make_async_copy(
            row_ref.at[:, pl.ds(width, cols - width)], panel.at[own_rows, pl.ds(width, cols - width)],
            load_sem.at[3])
    pl.semaphore_wait(barrier, 1 + y + x + jnp.where(z > 0, 1, 0))

    @pl.when(z > 0)
    def _():
        tell(0, down, mr)

    @pl.when(x == 1)
    def _():
        tell(1, across, mr)

    for k in range(pairs - 1):
        @pl.when(k < y)
        def _():
            tell(2, mc, 2 * k + core)

    def remote(ref, send, recv, mc_index, mr_index):
        return pltpu.make_async_remote_copy(
            src_ref=ref, dst_ref=ref, send_sem=send, recv_sem=recv,
            device_id=at(mc_index, mr_index), device_id_type=pl.DeviceIdType.MESH)

    def piece(shard, c, low=None, span=None):
        first = pl.multiple_of(shard * rows, rows)
        count = rows
        if low is not None:
            first = pl.multiple_of(shard * rows + low * half, half)
            count = half
        return panel.at[pl.ds(first, count), pl.ds(pl.multiple_of(c * width, width), span or width)]

    target = (down, up, across)

    def line(q, c, way, send=None, span=None):
        return remote(piece(2 * q + x, c, None, span), send_sem.at[way] if send is None else send,
                      line_recv.at[q - 1 if way == 0 else q, c], target[way], mr)

    def split_piece(c, way):
        return remote(piece((top, bottom)[way], c, 1), send_sem.at[way], half_recv.at[way, c], target[way], mr)

    def pair(shard, c, send=None, span=None):
        return remote(piece(shard, c, None, span), send_sem.at[2] if send is None else send,
                      pair_recv.at[c], across, mr)

    def cross(q, c, low=None):
        return remote(piece(2 * q + x, c, low), send_sem.at[2], rest_recv.at[c], across, mr)

    def diag_line(q, way):
        ref = diags.at[mr, pl.ds(pl.multiple_of((2 * q + x) * rows, rows), rows)]
        return remote(ref, diag_send.at[way], diag_recv.at[q if way < 2 else levels], target[way], mr)

    def block_copy(k, step):
        return remote(diags.at[k], block_send.at[0], block_recv.at[0], mc, lax.rem(mr + step, n_mr))

    def column_copy(k, step):
        return remote(columns.at[own_part(k)], col_send.at[0], col_recv.at[0], mc, lax.rem(mr + step, n_mr))

    def send_row(c):
        def send(span):
            send = own_send.at[0] if c == final else None

            @pl.when(z > 0)
            def _():
                line(z, c, 0, send, span).start()

            @pl.when(z < last)
            def _():
                line(z, c, 1, send, span).start()

            pair(mc, c, send, span).start()

        if c == final and detour:
            by_mr(lambda: send(kept), lambda: send(width))
        else:
            send(width)

    def by_mr(first, others):
        pl.when(mr == 0)(first)
        pl.when(mr != 0)(others)

    sides = (z > 0, z < last, None)

    def each_side(act):
        for way in range(3):
            if sides[way] is None:
                act(way)
            else:
                pl.when(sides[way])(functools.partial(act, way))

    def detoured(shard):
        return panel.at[pl.ds(pl.multiple_of(shard * rows, rows), rows), pl.ds(final * width + kept, detour)]

    def carry_out():
        return pltpu.make_async_remote_copy(
            src_ref=detoured(mc), dst_ref=carried.at[0], send_sem=carry_send.at[0], recv_sem=carry_recv.at[0],
            device_id=at(mc, n_mr - 1), device_id_type=pl.DeviceIdType.MESH)

    def carry_on(way):
        return pltpu.make_async_remote_copy(
            src_ref=carried.at[0], dst_ref=carried.at[1 + way], send_sem=carry_send.at[0],
            recv_sem=carry_recv.at[1 + way], device_id=at(target[way], mr), device_id_type=pl.DeviceIdType.MESH)

    def carry_home(way):
        shard = (mc + 2, mc - 2, across)[way]
        return pltpu.make_async_remote_copy(
            src_ref=carried.at[1 + way], dst_ref=detoured(shard), send_sem=carry_send.at[1],
            recv_sem=carry_recv.at[1 + way], device_id=at(mc, 0), device_id_type=pl.DeviceIdType.MESH)

    sources = (z < last, z > 0, None)

    def each_source(act):
        for way in range(3):
            if sources[way] is None:
                act(way)
            else:
                pl.when(sources[way])(functools.partial(act, way))

    def open_way(way):
        @pl.when(z < limit)
        def _():
            diag_line(z, way).start()

        send = own_send.at[0] if final == 0 else None
        (pair(mc, 0, send) if way == 2 else line(z, 0, way, send)).start()

    own_diag.wait()
    own_first.wait()

    @pl.when(z > 0)
    def _():
        open_way(0)

    @pl.when(x == 1)
    def _():
        open_way(2)

    if chunks > 1:
        own_rest.start()
    own_column.start()

    @pl.when(x == 0)
    def _():
        pl.semaphore_wait(ready_sem.at[1], 1)
        open_way(2)

    @pl.when(z < last)
    def _():
        pl.semaphore_wait(ready_sem.at[0], 1)
        open_way(1)

    @pl.when(y < pairs - 1)
    def _():
        pl.semaphore_wait(ready_sem.at[2], pairs - 1 - y)

    for k in range(1, pairs):
        @pl.when(k > y)
        def _():
            tell(3, mc, 2 * k + core)

    @pl.when(y > 0)
    def _():
        pl.semaphore_wait(ready_sem.at[3], y)

    if chunks > 1:
        own_rest.wait()
    if detour:
        @pl.when(mr == 0)
        def _():
            carry_out().start()
    own_column.wait()
    for step in range(1, n_mr):
        column_copy(mr, step).start()
    load_trailing = pltpu.make_async_copy(trailing_ref, updated_ref, trail_sem.at[0])
    load_trailing.start()

    for hop in range(last):
        above = z + 1 + hop
        below = z - 1 - hop

        @pl.when(above < limit)
        def _():
            diag_line(above, 0).wait_recv()

            @pl.when(z > 0)
            def _():
                diag_line(above, 0).start()

            diag_line(above, 2).start()

        @pl.when(jnp.logical_and(below >= 0, below < limit))
        def _():
            diag_line(below, 1).wait_recv()

            @pl.when(z < last)
            def _():
                diag_line(below, 1).start()

            diag_line(below, 2).start()

        if hop == 0 and detour:
            @pl.when(mr == n_mr - 1)
            def _():
                carry_out().wait_recv()
                each_side(lambda way: carry_on(way).start())
        if hop + 1 < chunks:
            send_row(hop + 1)
    for c in range(levels, chunks):
        send_row(c)
    if detour:
        @pl.when(mr == n_mr - 1)
        def _():
            def pass_home(way):
                carry_on(way).wait_recv()
                carry_home(way).start()

            each_source(pass_home)

    first_half_only = lambda q: jnp.logical_or(
        jnp.logical_and(q == last, z != last), jnp.logical_and(q == 0, z != 0))

    def send_across(q, c):
        @pl.when(first_half_only(q))
        def _():
            cross(q, c, 0).start()

        @pl.when(jnp.logical_not(first_half_only(q)))
        def _():
            cross(q, c).start()

    def invert():
        for m in range(n_mr):
            @pl.when(mr == m)
            def _():
                ref = diags.at[m, pl.ds(0, min(levels, (m + 1) * per) * rows)]
                remote(ref, diag_send.at[2], diag_recv.at[levels], across, mr).wait_recv()
        for step in range(1, n_mr):
            block_copy(mr, step).start()
        remote(diags.at[pl.ds(0, n_mr - 1)], block_send.at[0], block_recv.at[0], mc, lax.rem(mr + 1, n_mr)).wait_recv()
        for k in range(n_mr):
            matrix[:, k * block_cols:(k + 1) * block_cols] = diags[k]
        matrix[...] = upper_inverse(matrix[...])
        own_inverse = matrix[own_rows, :]
        remote(columns.at[pl.ds(0, (n_mr - 1) * block_cols)], col_send.at[0], col_recv.at[0], mc,
               lax.rem(mr + 1, n_mr)).wait_recv()
        flipped[...] = -lax.dot_general(
            matrix[...], columns[...], (((0,), (0,)), ((), ())),
            precision=HIGHEST, preferred_element_type=jnp.float32)
        solved_ref[...] = flipped[own_part(mr), :]
        left_high[0:height, :], left_low[0:height, :] = split(flipped[...].T)
        left_high[height:height + rows, :], left_low[height:height + rows, :] = split(own_inverse)
        for k in range(n_mr):
            @pl.when(mr == k)
            def _():
                inverse_ref[...] = own_inverse[:, k * block_cols:(k + 1) * block_cols]

    for phase in range(last):
        if phase == min(1, levels - 2):
            invert()

        above = z + 1 + phase
        below = z - 1 - phase

        def step(c, arrive):
            @pl.when(above < levels)
            def _():
                arrive(0, lambda span: line(above, c, 0, None, span))

                @pl.when(z > 0)
                def _():
                    line(above, c, 0).start()

                send_across(above, c)

            @pl.when(below >= 0)
            def _():
                arrive(1, lambda span: line(below, c, 1, None, span))

                @pl.when(z < last)
                def _():
                    line(below, c, 1).start()

                send_across(below, c)

            if phase == 0:
                arrive(2, lambda span: pair(2 * z + other, c, None, span))

                @pl.when(z == last)
                def _():
                    split_piece(c, 0).start()

                @pl.when(z == 0)
                def _():
                    split_piece(c, 1).start()

            @pl.when(above == levels)
            def _():
                @pl.when(z < last)
                def _():
                    split_piece(c, 0).wait_recv()

                    @pl.when(z > 0)
                    def _():
                        split_piece(c, 0).start()

            @pl.when(below == -1)
            def _():
                @pl.when(z > 0)
                def _():
                    split_piece(c, 1).wait_recv()

                    @pl.when(z < last)
                    def _():
                        split_piece(c, 1).start()

        def whole(way, make):
            make(width).wait_recv()

        def joined(way, make):
            def first():
                make(kept).wait_recv()
                carry_home(way).wait_recv()

            by_mr(first, lambda: make(width).wait_recv())

        split_last = phase == 0 and detour > 0
        pl.loop(0, chunks - 1 if split_last else chunks)(lambda c: step(c, whole))
        if split_last:
            step(final, joined)

    def receive_rest(c):
        @pl.when(z == 0)
        def _():
            split_piece(c, 0).wait_recv()

        @pl.when(z == last)
        def _():
            split_piece(c, 1).wait_recv()

        def gathered(halves):
            ref = panel.at[pl.ds(0, halves * half), pl.ds(0, width)]
            remote(ref, send_sem.at[2], rest_recv.at[c], across, mr).wait_recv()

        at_end = jnp.logical_or(z == 0, z == last)

        @pl.when(at_end)
        def _():
            gathered(2 * levels - 3)

        if levels > 2:
            @pl.when(jnp.logical_not(at_end))
            def _():
                gathered(2 * levels - 4)

    load_trailing.wait()

    @pl.loop(0, chunks - late)
    def _(c):
        receive_rest(c)
        for t in range(width // tile):
            part = pl.ds(pl.multiple_of(c * width + t * tile, tile), tile)
            product = multiply(left_high, left_low, panel[:, part])
            updated_ref[:, part] = updated_ref[:, part] + product[0:height]
            scaled_ref[:, part] = product[height:height + rows]

    for c in range(chunks - late, chunks):
        receive_rest(c)

    def sent(way, halves):
        ref = panel.at[pl.ds(0, halves * half - rows // chunks)]
        remote(ref, send_sem.at[way], pair_recv.at[0], target[way], mr).wait_send()

    def sent_own(count, span):
        ref = panel.at[pl.ds(0, count * rows), pl.ds(0, span)]
        remote(ref, own_send.at[0], pair_recv.at[0], across, mr).wait_send()

    def sent_diag(way, count):
        if count > 0:
            ref = diags.at[mr, pl.ds(0, count * rows)]
            remote(ref, diag_send.at[way], diag_recv.at[0], target[way], mr).wait_send()

    def sent_carry(slot, count):
        remote(carried.at[pl.ds(0, count)], carry_send.at[slot], carry_recv.at[0], across, mr).wait_send()

    for k in range(levels):
        @pl.when(z == k)
        def _():
            count = 1 + (k > 0) + (k < last)
            if k > 0:
                sent(0, 2 * (levels - k) + 1)
            if k < last:
                sent(1, 2 * (k + 1) + 1)
            sent(2, 2 * levels - (1 if k in (0, last) else 2))
            if detour:
                by_mr(lambda: sent_own(count, kept), lambda: sent_own(count, width))

                @pl.when(mr == n_mr - 1)
                def _():
                    sent_carry(0, count)
                    sent_carry(1, count)
            else:
                sent_own(count, width)
            for m in range(n_mr):
                @pl.when(mr == m)
                def _():
                    most = min(levels, (m + 1) * per)
                    if k > 0:
                        sent_diag(0, most - k)
                    if k < last:
                        sent_diag(1, min(k + 1, most))
                    sent_diag(2, most)

    if detour:
        @pl.when(mr == 0)
        def _():
            sent_carry(0, 1)

    remote(diags.at[pl.ds(0, n_mr - 1)], block_send.at[0], block_recv.at[0], mc, lax.rem(mr + 1, n_mr)).wait_send()
    remote(columns.at[pl.ds(0, (n_mr - 1) * block_cols)], col_send.at[0], col_recv.at[0], mc,
           lax.rem(mr + 1, n_mr)).wait_send()


def multiply(left_high, left_low, right):
    right_high, right_low = split(right)
    product = jnp.dot(left_high[...], right_low, preferred_element_type=jnp.float32)
    product += jnp.dot(left_low[...], right_high, preferred_element_type=jnp.float32)
    return product + jnp.dot(left_high[...], right_high, preferred_element_type=jnp.float32)


def finish(done, tile, solved, inverse, scaled, updated, panel, left_high, left_low,
           solved_out, inverse_out, scaled_out, updated_out, held_updated, held_scaled, sem):
    height, cols = updated.shape
    strips = 8
    deep = height // strips
    ready = pl.ds(0, done)
    rest = pl.ds(done, cols - done)
    for i in range(strips):
        part = pl.ds(i * deep, deep)
        pltpu.make_async_copy(updated.at[part, ready], updated_out.at[part, ready], sem.at[3]).start()
    copies = [
        pltpu.make_async_copy(solved, solved_out, sem.at[0]),
        pltpu.make_async_copy(inverse, inverse_out, sem.at[1]),
        pltpu.make_async_copy(scaled.at[:, ready], scaled_out.at[:, ready], sem.at[2]),
    ]
    for c in copies:
        c.start()
    copies.append(pltpu.make_async_copy(updated.at[:, ready], updated_out.at[:, ready], sem.at[3]))
    for t in range((cols - done) // tile):
        part = pl.ds(done + t * tile, tile)
        slot = pl.ds(t * tile, tile)
        product = multiply(left_high, left_low, panel[:, part])
        held_updated[:, slot] = updated[:, part] + product[0:height]
        held_scaled[:, slot] = product[height:]
        pltpu.make_async_copy(held_updated.at[:, slot], updated_out.at[:, part], sem.at[4]).start()
        pltpu.make_async_copy(held_scaled.at[:, slot], scaled_out.at[:, part], sem.at[5]).start()
    if done < cols:
        copies.append(pltpu.make_async_copy(held_updated, updated_out.at[:, rest], sem.at[4]))
        copies.append(pltpu.make_async_copy(held_scaled, scaled_out.at[:, rest], sem.at[5]))
    for c in copies:
        c.wait()


def shards(n_mc, n_mr, column_panel, diag_block, row_panel, trailing):
    rows, block_cols = diag_block.shape
    height, cols = trailing.shape
    order = rows * n_mc
    levels = n_mc // 2
    chunks = max(1, 16 // levels)
    while cols % (chunks * 128):
        chunks //= 2
    late = 1 if chunks > 1 else 0
    width = cols // chunks
    done = cols - late * width
    tile = 512 if width % 512 == 0 else 128
    detour = width // 1024 * 128 if n_mr > 1 and chunks > 1 and levels > 1 else 0
    held = 4 * (height * cols + rows * cols + block_cols * height + rows * 128 + order * cols
                + (height + rows) * order) + 64 * 1024
    dma = pltpu.SemaphoreType.DMA
    f32 = jnp.float32
    anywhere = pl.BlockSpec(memory_space=pl.ANY)
    vmem = pl.BlockSpec(memory_space=pltpu.VMEM)
    parts = pl.pallas_call(
        functools.partial(kernel, n_mc, n_mr, chunks, late, tile, detour),
        out_shape=(
            pltpu.VMEM((block_cols, height), f32),
            pltpu.VMEM(diag_block.shape, f32),
            pltpu.VMEM(row_panel.shape, f32),
            pltpu.VMEM(trailing.shape, f32),
            pltpu.VMEM((order, cols), f32),
            pltpu.VMEM((height + rows, order), jnp.bfloat16),
            pltpu.VMEM((height + rows, order), jnp.bfloat16),
        ),
        in_specs=[pl.BlockSpec(memory_space=pltpu.HBM)] * 4,
        out_specs=(vmem,) * 7,
        scratch_shapes=[
            pltpu.VMEM((order, height), f32),
            pltpu.VMEM((n_mr, order, block_cols), f32),
            pltpu.VMEM((order, order), f32),
            pltpu.VMEM((order, height), f32),
            pltpu.VMEM((4, rows, max(detour, 128)), f32),
            dma((4,)), dma((1,)), dma((3,)), dma((max(1, levels - 1), chunks)), dma((2, chunks)), dma((chunks,)), dma((chunks,)),
            dma((3,)), dma((levels + 1,)), dma((1,)), dma((1,)), dma((1,)), dma((1,)),
            dma((1,)), dma((2,)), dma((4,)), pltpu.SemaphoreType.REGULAR((4,)),
        ],
        compiler_params=pltpu.CompilerParams(
            collective_id=0, has_side_effects=True, vmem_limit_bytes=VMEM_BYTES - held),
    )(column_panel.T, diag_block, row_panel, trailing)
    spare = max(tile, cols - done)
    solved, inverse, scaled, updated = pl.pallas_call(
        functools.partial(finish, done, tile),
        out_shape=tuple(jax.ShapeDtypeStruct(part.shape, f32) for part in parts[:4]),
        in_specs=[vmem] * 7,
        out_specs=(anywhere,) * 4,
        scratch_shapes=[pltpu.VMEM((height, spare), f32), pltpu.VMEM((rows, spare), f32), dma((6,))],
        compiler_params=pltpu.CompilerParams(vmem_limit_bytes=4 * (height + rows) * (spare + 4 * tile) + 1024 * 1024),
    )(*parts)
    return solved.T, inverse, scaled, updated


def solution(mesh):
    placed = (P("mc", "mr"),) * 4
    return jax.shard_map(
        functools.partial(shards, mesh.shape["mc"], mesh.shape["mr"]),
        mesh=mesh, in_specs=placed, out_specs=placed, check_vma=False)
```

```python
import functools

import jax
import jax.numpy as jnp
from jax import lax
from jax.experimental import pallas as pl
from jax.experimental.pallas import tpu as pltpu
from jax.sharding import PartitionSpec as P

VMEM_BYTES = 67043328
HIGHEST = lax.Precision.HIGHEST


def dot(a, b):
    return jnp.dot(a, b, precision=HIGHEST, preferred_element_type=jnp.float32)


def upper_inverse(matrix):
    order = matrix.shape[0]
    row = lax.broadcasted_iota(jnp.int32, (order, order), 0)
    col = lax.broadcasted_iota(jnp.int32, (order, order), 1)
    on_diag = row == col
    pivots = jnp.where(on_diag, matrix, 0.0)
    recip_col = 1.0 / jnp.sum(pivots, axis=1, keepdims=True)
    recip_row = 1.0 / jnp.sum(pivots, axis=0, keepdims=True)
    power = -(recip_col * jnp.where(col > row, matrix, 0.0))
    identity = jnp.where(on_diag, 1.0, 0.0)
    product = identity + power
    steps = max((order - 1).bit_length(), 1)
    for level in range(steps - 1):
        power = dot(power, power)
        product = dot(product, identity + power)
    return product * recip_row


def split(value):
    high = value.astype(jnp.bfloat16)
    low = (value - high.astype(jnp.float32)).astype(jnp.bfloat16)
    return high, low


def kernel(n_mc, n_mr, chunks, late, tile, detour,
           column_ref, diag_ref, row_ref, trailing_ref,
           solved_ref, inverse_ref, scaled_ref, updated_ref, panel, left_high, left_low,
           columns, diags, matrix, flipped, carried,
           load_sem, trail_sem, send_sem, line_recv, half_recv, pair_recv, rest_recv,
           diag_send, diag_recv, block_send, block_recv, col_send, col_recv, own_send, carry_send, carry_recv,
           ready_sem):
    mc = lax.axis_index("mc")
    mr = lax.axis_index("mr")
    levels = n_mc // 2
    z = mc // 2
    x = lax.rem(mc, 2)
    rows = row_ref.shape[0]
    half = rows // 2
    cols = row_ref.shape[1]
    width = cols // chunks
    block_cols = diag_ref.shape[1]
    height = column_ref.shape[1]
    last = levels - 1
    final = chunks - 1
    kept = width - detour
    per = block_cols // (2 * rows) if block_cols % (2 * rows) == 0 else levels
    needed = lambda m: jnp.minimum(levels, (m + 1) * per)
    limit = needed(mr)

    def at(mc_index, mr_index):
        return {"mc": mc_index, "mr": mr_index}

    down = jnp.maximum(mc - 2, 0)
    up = jnp.minimum(mc + 2, n_mc - 1)
    across = z * 2 + 1 - x
    other = 1 - x
    top = 2 * last + other
    bottom = other

    barrier = pltpu.get_barrier_semaphore()

    def greet(mc_index, mr_index):
        pl.semaphore_signal(barrier, inc=1, device_id=at(mc_index, mr_index),
                            device_id_type=pl.DeviceIdType.MESH)

    pairs = n_mr // 2
    y = mr // 2
    core = lax.rem(mr, 2)

    def tell(sem, mc_index, mr_index):
        pl.semaphore_signal(ready_sem.at[sem], inc=1, device_id=at(mc_index, mr_index),
                            device_id_type=pl.DeviceIdType.MESH)

    @pl.when(z < last)
    def _():
        greet(up, mr)

    @pl.when(x == 0)
    def _():
        greet(across, mr)

    greet(mc, mr + 1 - 2 * core)
    for k in range(pairs):
        @pl.when(k > y)
        def _():
            greet(mc, 2 * k + core)

    own_rows = pl.ds(pl.multiple_of(mc * rows, rows), rows)
    own_part = lambda k: pl.ds(pl.multiple_of(k * block_cols, block_cols), block_cols)
    own_diag = pltpu.make_async_copy(diag_ref, diags.at[mr, own_rows], load_sem.at[0])
    own_column = pltpu.make_async_copy(column_ref, columns.at[own_part(mr)], load_sem.at[1])
    own_first = pltpu.make_async_copy(
        row_ref.at[:, pl.ds(0, width)], panel.at[own_rows, pl.ds(0, width)], load_sem.at[2])
    own_diag.start()
    own_first.start()
    if chunks > 1:
        own_rest = pltpu.make_async_copy(
            row_ref.at[:, pl.ds(width, cols - width)], panel.at[own_rows, pl.ds(width, cols - width)],
            load_sem.at[3])
    pl.semaphore_wait(barrier, 1 + y + x + jnp.where(z > 0, 1, 0))

    @pl.when(z > 0)
    def _():
        tell(0, down, mr)

    @pl.when(x == 1)
    def _():
        tell(1, across, mr)

    for k in range(pairs - 1):
        @pl.when(k < y)
        def _():
            tell(2, mc, 2 * k + core)

    def remote(ref, send, recv, mc_index, mr_index):
        return pltpu.make_async_remote_copy(
            src_ref=ref, dst_ref=ref, send_sem=send, recv_sem=recv,
            device_id=at(mc_index, mr_index), device_id_type=pl.DeviceIdType.MESH)

    def piece(shard, c, low=None, span=None):
        first = pl.multiple_of(shard * rows, rows)
        count = rows
        if low is not None:
            first = pl.multiple_of(shard * rows + low * half, half)
            count = half
        return panel.at[pl.ds(first, count), pl.ds(pl.multiple_of(c * width, width), span or width)]

    target = (down, up, across)

    def line(q, c, way, send=None, span=None):
        return remote(piece(2 * q + x, c, None, span), send_sem.at[way] if send is None else send,
                      line_recv.at[q - 1 if way == 0 else q, c], target[way], mr)

    def split_piece(c, way):
        return remote(piece((top, bottom)[way], c, 1), send_sem.at[way], half_recv.at[way, c], target[way], mr)

    def pair(shard, c, send=None, span=None):
        return remote(piece(shard, c, None, span), send_sem.at[2] if send is None else send,
                      pair_recv.at[c], across, mr)

    def cross(q, c, low=None):
        return remote(piece(2 * q + x, c, low), send_sem.at[2], rest_recv.at[c], across, mr)

    def diag_line(q, way):
        ref = diags.at[mr, pl.ds(pl.multiple_of((2 * q + x) * rows, rows), rows)]
        return remote(ref, diag_send.at[way], diag_recv.at[q if way < 2 else levels], target[way], mr)

    def block_copy(k, step):
        return remote(diags.at[k], block_send.at[0], block_recv.at[0], mc, lax.rem(mr + step, n_mr))

    def column_copy(k, step):
        return remote(columns.at[own_part(k)], col_send.at[0], col_recv.at[0], mc, lax.rem(mr + step, n_mr))

    def send_row(c):
        def make(way, send, span=None):
            return pair(mc, c, send, span) if way == 2 else line(z, c, way, send, span)

        def send(way):
            if c != final:
                make(way, None).start()
            elif not detour or way == 1:
                make(way, own_send.at[0]).start()
            else:
                trimmed = jnp.logical_and(mr == 0, x == (0 if way == 0 else 1))
                pl.when(trimmed)(lambda: make(way, own_send.at[1], kept).start())
                pl.when(jnp.logical_not(trimmed))(lambda: make(way, own_send.at[0]).start())

        each_side(send)

    sides = (z > 0, z < last, None)

    def each_side(act):
        for way in range(3):
            if sides[way] is None:
                act(way)
            else:
                pl.when(sides[way])(functools.partial(act, way))

    def detoured(shard):
        return panel.at[pl.ds(pl.multiple_of(shard * rows, rows), rows), pl.ds(final * width + kept, detour)]

    def carry_out():
        return pltpu.make_async_remote_copy(
            src_ref=detoured(mc), dst_ref=carried.at[0], send_sem=carry_send.at[0], recv_sem=carry_recv.at[0],
            device_id=at(mc, n_mr - 1), device_id_type=pl.DeviceIdType.MESH)

    def carry_on(way):
        return pltpu.make_async_remote_copy(
            src_ref=carried.at[0], dst_ref=carried.at[1 + way], send_sem=carry_send.at[0],
            recv_sem=carry_recv.at[1 + way], device_id=at(target[way], mr), device_id_type=pl.DeviceIdType.MESH)

    def carry_home(way):
        shard = (mc + 2, mc - 2, across)[way]
        return pltpu.make_async_remote_copy(
            src_ref=carried.at[1 + way], dst_ref=detoured(shard), send_sem=carry_send.at[1],
            recv_sem=carry_recv.at[1 + way], device_id=at(mc, 0), device_id_type=pl.DeviceIdType.MESH)

    def open_way(way):
        @pl.when(z < limit)
        def _():
            diag_line(z, way).start()

        send = own_send.at[0] if final == 0 else None
        (pair(mc, 0, send) if way == 2 else line(z, 0, way, send)).start()

    own_diag.wait()
    own_first.wait()

    @pl.when(z > 0)
    def _():
        open_way(0)

    @pl.when(x == 1)
    def _():
        open_way(2)

    if chunks > 1:
        own_rest.start()
    own_column.start()

    @pl.when(x == 0)
    def _():
        pl.semaphore_wait(ready_sem.at[1], 1)
        open_way(2)

    @pl.when(z < last)
    def _():
        pl.semaphore_wait(ready_sem.at[0], 1)
        open_way(1)

    @pl.when(y < pairs - 1)
    def _():
        pl.semaphore_wait(ready_sem.at[2], pairs - 1 - y)

    for k in range(1, pairs):
        @pl.when(k > y)
        def _():
            tell(3, mc, 2 * k + core)

    @pl.when(y > 0)
    def _():
        pl.semaphore_wait(ready_sem.at[3], y)

    if chunks > 1:
        own_rest.wait()
    if detour:
        @pl.when(mr == 0)
        def _():
            carry_out().start()
    own_column.wait()
    for step in range(1, n_mr):
        column_copy(mr, step).start()
    load_trailing = pltpu.make_async_copy(trailing_ref, updated_ref, trail_sem.at[0])
    load_trailing.start()

    for hop in range(last):
        above = z + 1 + hop
        below = z - 1 - hop

        @pl.when(above < limit)
        def _():
            diag_line(above, 0).wait_recv()

            @pl.when(z > 0)
            def _():
                diag_line(above, 0).start()

            diag_line(above, 2).start()

        @pl.when(jnp.logical_and(below >= 0, below < limit))
        def _():
            diag_line(below, 1).wait_recv()

            @pl.when(z < last)
            def _():
                diag_line(below, 1).start()

            diag_line(below, 2).start()

        if hop == 0 and detour:
            @pl.when(mr == n_mr - 1)
            def _():
                carry_out().wait_recv()

                @pl.when(jnp.logical_and(z > 0, x == 0))
                def _():
                    carry_on(0).start()

                @pl.when(x == 1)
                def _():
                    carry_on(2).start()
        if hop + 1 < chunks:
            send_row(hop + 1)
    for c in range(levels, chunks):
        send_row(c)
    if detour:
        @pl.when(mr == n_mr - 1)
        def _():
            def pass_home(way):
                carry_on(way).wait_recv()
                carry_home(way).start()

            @pl.when(jnp.logical_and(z < last, x == 0))
            def _():
                pass_home(0)

            @pl.when(x == 0)
            def _():
                pass_home(2)

    first_half_only = lambda q: jnp.logical_or(
        jnp.logical_and(q == last, z != last), jnp.logical_and(q == 0, z != 0))

    def send_across(q, c):
        @pl.when(first_half_only(q))
        def _():
            cross(q, c, 0).start()

        @pl.when(jnp.logical_not(first_half_only(q)))
        def _():
            cross(q, c).start()

    def invert():
        for m in range(n_mr):
            @pl.when(mr == m)
            def _():
                ref = diags.at[m, pl.ds(0, min(levels, (m + 1) * per) * rows)]
                remote(ref, diag_send.at[2], diag_recv.at[levels], across, mr).wait_recv()
        for step in range(1, n_mr):
            block_copy(mr, step).start()
        remote(diags.at[pl.ds(0, n_mr - 1)], block_send.at[0], block_recv.at[0], mc, lax.rem(mr + 1, n_mr)).wait_recv()
        for k in range(n_mr):
            matrix[:, k * block_cols:(k + 1) * block_cols] = diags[k]
        matrix[...] = upper_inverse(matrix[...])
        own_inverse = matrix[own_rows, :]
        remote(columns.at[pl.ds(0, (n_mr - 1) * block_cols)], col_send.at[0], col_recv.at[0], mc,
               lax.rem(mr + 1, n_mr)).wait_recv()
        flipped[...] = -lax.dot_general(
            matrix[...], columns[...], (((0,), (0,)), ((), ())),
            precision=HIGHEST, preferred_element_type=jnp.float32)
        solved_ref[...] = flipped[own_part(mr), :]
        left_high[0:height, :], left_low[0:height, :] = split(flipped[...].T)
        left_high[height:height + rows, :], left_low[height:height + rows, :] = split(own_inverse)
        for k in range(n_mr):
            @pl.when(mr == k)
            def _():
                inverse_ref[...] = own_inverse[:, k * block_cols:(k + 1) * block_cols]

    for phase in range(last):
        if phase == min(1, levels - 2):
            invert()

        above = z + 1 + phase
        below = z - 1 - phase

        def step(c, arrive):
            @pl.when(above < levels)
            def _():
                arrive(0, lambda span: line(above, c, 0, None, span))

                @pl.when(z > 0)
                def _():
                    line(above, c, 0).start()

                send_across(above, c)

            @pl.when(below >= 0)
            def _():
                arrive(1, lambda span: line(below, c, 1, None, span))

                @pl.when(z < last)
                def _():
                    line(below, c, 1).start()

                send_across(below, c)

            if phase == 0:
                arrive(2, lambda span: pair(2 * z + other, c, None, span))

                @pl.when(z == last)
                def _():
                    split_piece(c, 0).start()

                @pl.when(z == 0)
                def _():
                    split_piece(c, 1).start()

            @pl.when(above == levels)
            def _():
                @pl.when(z < last)
                def _():
                    split_piece(c, 0).wait_recv()

                    @pl.when(z > 0)
                    def _():
                        split_piece(c, 0).start()

            @pl.when(below == -1)
            def _():
                @pl.when(z > 0)
                def _():
                    split_piece(c, 1).wait_recv()

                    @pl.when(z < last)
                    def _():
                        split_piece(c, 1).start()

        def whole(way, make):
            make(width).wait_recv()

        def joined(way, make):
            def first():
                make(kept).wait_recv()
                carry_home(way).wait_recv()

            if way == 1:
                make(width).wait_recv()
            else:
                both = jnp.logical_and(mr == 0, x == 0)
                pl.when(both)(first)
                pl.when(jnp.logical_not(both))(lambda: make(width).wait_recv())

        split_last = phase == 0 and detour > 0
        pl.loop(0, chunks - 1 if split_last else chunks)(lambda c: step(c, whole))
        if split_last:
            step(final, joined)

    def receive_rest(c):
        @pl.when(z == 0)
        def _():
            split_piece(c, 0).wait_recv()

        @pl.when(z == last)
        def _():
            split_piece(c, 1).wait_recv()

        def gathered(halves):
            ref = panel.at[pl.ds(0, halves * half), pl.ds(0, width)]
            remote(ref, send_sem.at[2], rest_recv.at[c], across, mr).wait_recv()

        at_end = jnp.logical_or(z == 0, z == last)

        @pl.when(at_end)
        def _():
            gathered(2 * levels - 3)

        if levels > 2:
            @pl.when(jnp.logical_not(at_end))
            def _():
                gathered(2 * levels - 4)

    load_trailing.wait()

    @pl.loop(0, chunks - late)
    def _(c):
        receive_rest(c)
        for t in range(width // tile):
            part = pl.ds(pl.multiple_of(c * width + t * tile, tile), tile)
            product = multiply(left_high, left_low, panel[:, part])
            updated_ref[:, part] = updated_ref[:, part] + product[0:height]
            scaled_ref[:, part] = product[height:height + rows]

    for c in range(chunks - late, chunks):
        receive_rest(c)

    def sent(way, halves):
        ref = panel.at[pl.ds(0, halves * half - rows // chunks)]
        remote(ref, send_sem.at[way], pair_recv.at[0], target[way], mr).wait_send()

    def sent_own(count, span, sem=0):
        ref = panel.at[pl.ds(0, count * rows), pl.ds(0, span)]
        remote(ref, own_send.at[sem], pair_recv.at[0], across, mr).wait_send()

    def sent_diag(way, count):
        if count > 0:
            ref = diags.at[mr, pl.ds(0, count * rows)]
            remote(ref, diag_send.at[way], diag_recv.at[0], target[way], mr).wait_send()

    def sent_carry(slot, count):
        remote(carried.at[pl.ds(0, count)], carry_send.at[slot], carry_recv.at[0], across, mr).wait_send()

    for k in range(levels):
        @pl.when(z == k)
        def _():
            count = 1 + (k > 0) + (k < last)
            if k > 0:
                sent(0, 2 * (levels - k) + 1)
            if k < last:
                sent(1, 2 * (k + 1) + 1)
            sent(2, 2 * levels - (1 if k in (0, last) else 2))
            if detour:
                for side in range(2):
                    trims = 1 if side == 1 or k > 0 else 0

                    @pl.when(jnp.logical_and(mr == 0, x == side))
                    def _():
                        sent_own(count - trims, width)
                        if trims:
                            sent_own(trims, kept, 1)

                    @pl.when(jnp.logical_and(mr == n_mr - 1, x == side))
                    def _():
                        if trims:
                            sent_carry(0, trims)
                        if side == 0:
                            sent_carry(1, 1 + (k < last))

                @pl.when(mr != 0)
                def _():
                    sent_own(count, width)
            else:
                sent_own(count, width)
            for m in range(n_mr):
                @pl.when(mr == m)
                def _():
                    most = min(levels, (m + 1) * per)
                    if k > 0:
                        sent_diag(0, most - k)
                    if k < last:
                        sent_diag(1, min(k + 1, most))
                    sent_diag(2, most)

    if detour:
        @pl.when(mr == 0)
        def _():
            sent_carry(0, 1)

    remote(diags.at[pl.ds(0, n_mr - 1)], block_send.at[0], block_recv.at[0], mc, lax.rem(mr + 1, n_mr)).wait_send()
    remote(columns.at[pl.ds(0, (n_mr - 1) * block_cols)], col_send.at[0], col_recv.at[0], mc,
           lax.rem(mr + 1, n_mr)).wait_send()


def multiply(left_high, left_low, right):
    right_high, right_low = split(right)
    product = jnp.dot(left_high[...], right_low, preferred_element_type=jnp.float32)
    product += jnp.dot(left_low[...], right_high, preferred_element_type=jnp.float32)
    return product + jnp.dot(left_high[...], right_high, preferred_element_type=jnp.float32)


def finish(done, tile, solved, inverse, scaled, updated, panel, left_high, left_low,
           solved_out, inverse_out, scaled_out, updated_out, held_updated, held_scaled, sem):
    height, cols = updated.shape
    strips = 8
    deep = height // strips
    ready = pl.ds(0, done)
    rest = pl.ds(done, cols - done)
    for i in range(strips):
        part = pl.ds(i * deep, deep)
        pltpu.make_async_copy(updated.at[part, ready], updated_out.at[part, ready], sem.at[3]).start()
    copies = [
        pltpu.make_async_copy(solved, solved_out, sem.at[0]),
        pltpu.make_async_copy(inverse, inverse_out, sem.at[1]),
        pltpu.make_async_copy(scaled.at[:, ready], scaled_out.at[:, ready], sem.at[2]),
    ]
    for c in copies:
        c.start()
    copies.append(pltpu.make_async_copy(updated.at[:, ready], updated_out.at[:, ready], sem.at[3]))
    for t in range((cols - done) // tile):
        part = pl.ds(done + t * tile, tile)
        slot = pl.ds(t * tile, tile)
        product = multiply(left_high, left_low, panel[:, part])
        held_updated[:, slot] = updated[:, part] + product[0:height]
        held_scaled[:, slot] = product[height:]
        pltpu.make_async_copy(held_updated.at[:, slot], updated_out.at[:, part], sem.at[4]).start()
        pltpu.make_async_copy(held_scaled.at[:, slot], scaled_out.at[:, part], sem.at[5]).start()
    if done < cols:
        copies.append(pltpu.make_async_copy(held_updated, updated_out.at[:, rest], sem.at[4]))
        copies.append(pltpu.make_async_copy(held_scaled, scaled_out.at[:, rest], sem.at[5]))
    for c in copies:
        c.wait()


def shards(n_mc, n_mr, column_panel, diag_block, row_panel, trailing):
    rows, block_cols = diag_block.shape
    height, cols = trailing.shape
    order = rows * n_mc
    levels = n_mc // 2
    chunks = max(1, 16 // levels)
    while cols % (chunks * 128):
        chunks //= 2
    late = 1 if chunks > 1 else 0
    width = cols // chunks
    done = cols - late * width
    tile = 512 if width % 512 == 0 else 128
    detour = width // 1024 * 128 if n_mr > 1 and chunks > 1 and levels > 1 else 0
    held = 4 * (height * cols + rows * cols + block_cols * height + rows * 128 + order * cols
                + (height + rows) * order) + 64 * 1024
    dma = pltpu.SemaphoreType.DMA
    f32 = jnp.float32
    anywhere = pl.BlockSpec(memory_space=pl.ANY)
    vmem = pl.BlockSpec(memory_space=pltpu.VMEM)
    parts = pl.pallas_call(
        functools.partial(kernel, n_mc, n_mr, chunks, late, tile, detour),
        out_shape=(
            pltpu.VMEM((block_cols, height), f32),
            pltpu.VMEM(diag_block.shape, f32),
            pltpu.VMEM(row_panel.shape, f32),
            pltpu.VMEM(trailing.shape, f32),
            pltpu.VMEM((order, cols), f32),
            pltpu.VMEM((height + rows, order), jnp.bfloat16),
            pltpu.VMEM((height + rows, order), jnp.bfloat16),
        ),
        in_specs=[pl.BlockSpec(memory_space=pltpu.HBM)] * 4,
        out_specs=(vmem,) * 7,
        scratch_shapes=[
            pltpu.VMEM((order, height), f32),
            pltpu.VMEM((n_mr, order, block_cols), f32),
            pltpu.VMEM((order, order), f32),
            pltpu.VMEM((order, height), f32),
            pltpu.VMEM((4, rows, max(detour, 128)), f32),
            dma((4,)), dma((1,)), dma((3,)), dma((max(1, levels - 1), chunks)), dma((2, chunks)), dma((chunks,)), dma((chunks,)),
            dma((3,)), dma((levels + 1,)), dma((1,)), dma((1,)), dma((1,)), dma((1,)),
            dma((2,)), dma((2,)), dma((4,)), pltpu.SemaphoreType.REGULAR((4,)),
        ],
        compiler_params=pltpu.CompilerParams(
            collective_id=0, has_side_effects=True, vmem_limit_bytes=VMEM_BYTES - held),
    )(column_panel.T, diag_block, row_panel, trailing)
    spare = max(tile, cols - done)
    solved, inverse, scaled, updated = pl.pallas_call(
        functools.partial(finish, done, tile),
        out_shape=tuple(jax.ShapeDtypeStruct(part.shape, f32) for part in parts[:4]),
        in_specs=[vmem] * 7,
        out_specs=(anywhere,) * 4,
        scratch_shapes=[pltpu.VMEM((height, spare), f32), pltpu.VMEM((rows, spare), f32), dma((6,))],
        compiler_params=pltpu.CompilerParams(vmem_limit_bytes=4 * (height + rows) * (spare + 4 * tile) + 1024 * 1024),
    )(*parts)
    return solved.T, inverse, scaled, updated


def solution(mesh):
    placed = (P("mc", "mr"),) * 4
    return jax.shard_map(
        functools.partial(shards, mesh.shape["mc"], mesh.shape["mr"]),
        mesh=mesh, in_specs=placed, out_specs=placed, check_vma=False)
```
